32 devices in a mesh: period: 2 (over y), gx: 4 (over z), gy: 2 (over x), gz: 2 (over core).
Axes of the slice: x: 2, y: 2, z: 4, core: 2. Of those that a mesh axis runs over, the one named last changes fastest.
Arguments:
- residual: float32 [4, 3, 16, 16, 256], P('period', None, 'gx', 'gy', 'gz'), parts along dimension 0, may hold values from -6 to 6
- classes: int32 [16, 16, 256], P('gx', 'gy', 'gz'), may hold values from 0 to 15
- edge_mask: int32 [3, 16, 16, 256], P(None, 'gx', 'gy', 'gz'), may hold values from 0 to 1
- class_weight: float32 [32], P('period'), parts along dimension 0, may hold values from 0.01 to 1
Outputs:
- preconditioned: float32 [4, 3, 16, 16, 256], P('period', None, 'gx', 'gy', 'gz'), parts along dimension 0
The draws below stay inside these ranges and needn't reach their ends.
There are 2 independent parts, one for each index of `period`. The reference program is written for one: setup_inputs(seed, part) draws one part's arguments, and reference() takes and returns one part's arrays. A program takes and returns all parts, laid end to end along the dimension named above; an argument that names none is the same for every part. Nothing has to cross between parts.
All inputs are finite; a program needn't handle non-finite values.
Results may differ from the reference program's by a relative error of at most 0.00025.
Values sent between devices are 32-bit elements; how exact they have to be, the bound alone decides.
A program may use at most 64 MiB of HBM per device.

```python
import math
import jax
import jax.numpy as jnp
from jax import lax

COARSE_SWEEPS = 2
NCLASS = 16
NX = 16
NY = 16
NZ = 256


def draw_edge_mask(key, part):
    base_key, row_key, depth_key, row_pick, depth_pick = jax.random.split(jax.random.fold_in(key, 11), 5)
    scattered = (jax.random.randint(base_key, (3, NX, NY, NZ), 0, 16) == 0).astype(jnp.int32)
    row_blocks = (jax.random.randint(row_key, (NY // 4,), 0, 4) == 0).astype(jnp.int32)
    row_forced = (jnp.arange(NY // 4, dtype=jnp.int32) == jax.random.randint(row_pick, (), 0, NY // 4)).astype(jnp.int32)
    row_quiet = jnp.repeat(jnp.maximum(row_blocks, row_forced), 4)
    depth_blocks = (jax.random.randint(depth_key, (NZ // 4,), 0, 4) == 0).astype(jnp.int32)
    depth_forced = (jnp.arange(NZ // 4, dtype=jnp.int32) == jax.random.randint(depth_pick, (), 0, NZ // 4)).astype(jnp.int32)
    depth_quiet = jnp.repeat(jnp.maximum(depth_blocks, depth_forced), 4)
    quiet_cells = row_quiet[:, None] * depth_quiet[None, :]
    along_edges = scattered[0] * (1 - quiet_cells)[None]
    across_edges = jnp.maximum(scattered[1:], quiet_cells[None, None])
    return jnp.concatenate([along_edges[None], across_edges], axis=0)


def set_ends(values, key, low, top_value):
    longest = values.shape.index(max(values.shape))
    spots = []
    for shift in (0, 1):
        where = [jax.random.randint(jax.random.fold_in(key, axis), (), 0, length) for axis, length in enumerate(values.shape)]
        where[longest] = (where[longest] + shift) % values.shape[longest]
        spots.append(tuple(where))
    return values.at[spots[0]].set(low).at[spots[1]].set(top_value)


def block_levels(stream_key, extent, pieces, smallest, top_value):
    level, own = 1.0, jax.random.fold_in(stream_key, 6)
    for position, blocks in pieces:
        heights = jnp.exp(jax.random.uniform(jax.random.fold_in(own, position), (blocks,), jnp.float32, smallest / len(pieces), top_value / len(pieces)))
        level = level * jnp.repeat(heights, extent[position] // blocks).reshape([-1 if axis == position else 1 for axis in range(len(extent))])
    return level


def bell_draw(stream_key, shape, deviation, bound, cuts=(), held_as=jnp.bfloat16):
    gain = block_levels(stream_key, shape, cuts, -0.22, 0.18) if cuts else 1.0
    values = jax.random.normal(stream_key, shape, jnp.float32) * deviation * gain
    return jnp.minimum(jnp.maximum(values, -bound), bound).astype(held_as)


def setup_inputs(seed: int = 0, part: int = 0) -> dict:
    splits = jax.random.split(jax.random.key(seed), 5)
    own_keys = jax.random.split(jax.random.fold_in(splits[4], part), 5)
    residual = bell_draw(own_keys[0], (2, 3, NX, NY, NZ), 1.0, 6.0, ((2, 4), (3, 2), (4, 2)), jnp.float32)
    classes = set_ends(jax.random.randint(splits[1], (NX, NY, NZ), 0, NCLASS), jax.random.fold_in(splits[1], 1), 0, NCLASS - 1).astype(jnp.int32)
    edge_mask = draw_edge_mask(jax.random.fold_in(splits[4], 71), part)
    class_weight = jnp.clip(jnp.exp(jax.random.uniform(own_keys[3], (NCLASS,), jnp.float32, math.log(0.01), math.log(1.0))), 0.01, 1.0)
    return dict(residual=residual, classes=classes, edge_mask=edge_mask, class_weight=class_weight)


aspect = 2.0
face_weight = (1.0 / (aspect * aspect), 1.0, 1.0)
mass_factor = (aspect * aspect, 1.0, 1.0)
stiff_weight = (2.0 * (face_weight[1] + face_weight[2]), 2.0 * (face_weight[0] + face_weight[2]), 2.0 * (face_weight[0] + face_weight[1]))
edge_damping = 0.6
shift_ratio = 1.0e-4
shift_added = 0.05
coarse_along = 0.5625
coarse_across = 0.1875


def shifted(values, axis_index, offset):
    axis_index = axis_index % values.ndim
    length = values.shape[axis_index]
    widths = [(0, 0)] * values.ndim
    if offset > 0:
        widths[axis_index] = (0, 1)
        return lax.slice_in_dim(jnp.pad(values, widths), 1, length + 1, axis=axis_index)
    widths[axis_index] = (1, 0)
    return lax.slice_in_dim(jnp.pad(values, widths), 0, length, axis=axis_index)


def spread(per_kind):
    scalar_kind = per_kind[0:1]
    vector_kind = per_kind[1:2]
    return jnp.concatenate([scalar_kind, vector_kind, vector_kind, vector_kind], axis=0)


def edge_coefficients(cell_values, free_edges):
    cells_west = shifted(cell_values, 0, -1)
    cells_south = shifted(cell_values, 1, -1)
    cells_above = shifted(cell_values, 2, -1)
    first_edges = 0.25 * (((cell_values + cells_south) + cells_above) + shifted(cells_above, 1, -1))
    second_edges = 0.25 * (((cell_values + cells_west) + cells_above) + shifted(cells_above, 0, -1))
    third_edges = 0.25 * (((cell_values + cells_west) + cells_south) + shifted(cells_south, 0, -1))
    averages = jnp.stack([first_edges, second_edges, third_edges])
    factors = jnp.array(mass_factor, jnp.float32).reshape(3, 1, 1, 1)
    stiffness = jnp.array(stiff_weight, jnp.float32).reshape(3, 1, 1, 1)
    masses = factors * averages * free_edges
    edge_diagonal = stiffness + masses
    kind_weights = jnp.stack([masses, edge_diagonal * free_edges])
    return masses, edge_diagonal, kind_weights


def make_level(kind_weights):
    to_east = kind_weights[:, 0]
    to_north = kind_weights[:, 1]
    to_deep = kind_weights[:, 2]
    to_west = shifted(to_east, -3, -1)
    to_south = shifted(to_north, -2, -1)
    to_shallow = shifted(to_deep, -1, -1)
    weight_sum = ((((to_east + to_west) + to_north) + to_south) + to_deep) + to_shallow
    return (to_east, to_north, to_deep, to_west, to_south, to_shallow, (1.0 + shift_ratio) * weight_sum + shift_added)


def coarse_weights(kind_weights):
    grouped = kind_weights.reshape(kind_weights.shape[:3] + (kind_weights.shape[3] // 2, 2, kind_weights.shape[4] // 2, 2))
    summed = (grouped[:, :, :, :, 0, :, 0] + grouped[:, :, :, :, 1, :, 0]) + (grouped[:, :, :, :, 0, :, 1] + grouped[:, :, :, :, 1, :, 1])
    factors = jnp.array([coarse_along, coarse_across, coarse_across], jnp.float32).reshape(1, 3, 1, 1, 1)
    return summed * factors


def pad_space(values):
    return jnp.pad(values, ((0, 0), (0, 0), (1, 1), (1, 1), (1, 1)))


def curl_apply(padded, masses):
    extent_east = padded.shape[2] - 2
    extent_north = padded.shape[3] - 2
    extent_deep = padded.shape[4] - 2

    def region(values, move_east, move_north, move_deep, extra_cells):
        return values[:, move_east:move_east + extent_east + extra_cells, move_north:move_north + extent_north + extra_cells, move_deep:move_deep + extent_deep + extra_cells]

    field_east = padded[:, 0]
    field_north = padded[:, 1]
    field_deep = padded[:, 2]
    flux_east = face_weight[0] * ((region(field_deep, 0, 1, 0, 1) - region(field_deep, 0, 0, 0, 1)) - (region(field_north, 0, 0, 1, 1) - region(field_north, 0, 0, 0, 1)))
    flux_north = face_weight[1] * ((region(field_east, 0, 0, 1, 1) - region(field_east, 0, 0, 0, 1)) - (region(field_deep, 1, 0, 0, 1) - region(field_deep, 0, 0, 0, 1)))
    flux_deep = face_weight[2] * ((region(field_north, 1, 0, 0, 1) - region(field_north, 0, 0, 0, 1)) - (region(field_east, 0, 1, 0, 1) - region(field_east, 0, 0, 0, 1)))
    out_east = ((region(flux_north, 1, 1, 0, 0) - region(flux_north, 1, 1, 1, 0)) - (region(flux_deep, 1, 0, 1, 0) - region(flux_deep, 1, 1, 1, 0))) + masses[0] * region(field_east, 1, 1, 1, 0)
    out_north = ((region(flux_deep, 0, 1, 1, 0) - region(flux_deep, 1, 1, 1, 0)) - (region(flux_east, 1, 1, 0, 0) - region(flux_east, 1, 1, 1, 0))) + masses[1] * region(field_north, 1, 1, 1, 0)
    out_deep = ((region(flux_east, 1, 0, 1, 0) - region(flux_east, 1, 1, 1, 0)) - (region(flux_north, 0, 1, 1, 0) - region(flux_north, 1, 1, 1, 0))) + masses[2] * region(field_deep, 1, 1, 1, 0)
    return jnp.stack([out_east, out_north, out_deep], axis=1)


def side_padded(plane_pad, grid_level):
    return ((spread(grid_level[1]) * plane_pad[..., 2:, 1:-1] + spread(grid_level[4]) * plane_pad[..., :-2, 1:-1]) + spread(grid_level[2]) * plane_pad[..., 1:-1, 2:]) + spread(grid_level[5]) * plane_pad[..., 1:-1, :-2]


def apply_padded(padded, grid_level):
    center = padded[:, :, 1:-1, 1:-1, 1:-1]
    along_line = spread(grid_level[0]) * padded[:, :, 2:, 1:-1, 1:-1] + spread(grid_level[3]) * padded[:, :, :-2, 1:-1, 1:-1]
    return spread(grid_level[6]) * center - (along_line + side_padded(padded[:, :, 1:-1], grid_level))


def gradient_adjoint(padded):
    interior = padded[:, :, 1:-1, 1:-1, 1:-1]
    from_west = padded[:, 0, :-2, 1:-1, 1:-1]
    from_south = padded[:, 1, 1:-1, :-2, 1:-1]
    from_above = padded[:, 2, 1:-1, 1:-1, :-2]
    total_flow = ((from_west - interior[:, 0]) + (from_south - interior[:, 1])) + (from_above - interior[:, 2])
    return total_flow[:, None]


def average_adjoint(padded):
    interior = padded[:, :, 1:-1, 1:-1, 1:-1]
    return jnp.stack([0.5 * (interior[:, 0] + padded[:, 0, :-2, 1:-1, 1:-1]), 0.5 * (interior[:, 1] + padded[:, 1, 1:-1, :-2, 1:-1]), 0.5 * (interior[:, 2] + padded[:, 2, 1:-1, 1:-1, :-2])], axis=1)


def gradient_edges(padded):
    interior = padded[:, 0, 1:-1, 1:-1, 1:-1]
    return jnp.stack([padded[:, 0, 2:, 1:-1, 1:-1] - interior, padded[:, 0, 1:-1, 2:, 1:-1] - interior, padded[:, 0, 1:-1, 1:-1, 2:] - interior], axis=1)


def average_edges(padded):
    return jnp.stack([0.5 * (padded[:, 1, 1:-1, 1:-1, 1:-1] + padded[:, 1, 2:, 1:-1, 1:-1]), 0.5 * (padded[:, 2, 1:-1, 1:-1, 1:-1] + padded[:, 2, 1:-1, 2:, 1:-1]), 0.5 * (padded[:, 3, 1:-1, 1:-1, 1:-1] + padded[:, 3, 1:-1, 1:-1, 2:])], axis=1)


def restrict_plane(padded):
    extent_north = padded.shape[3] - 2
    extent_deep = padded.shape[4] - 2
    halved = padded[:, :, :, 1:extent_north + 1:2] + 0.5 * (padded[:, :, :, 0:extent_north:2] + padded[:, :, :, 2:extent_north + 2:2])
    return halved[..., 1:extent_deep + 1:2] + 0.5 * (halved[..., 0:extent_deep:2] + halved[..., 2:extent_deep + 2:2])


def prolong_plane(padded):
    extent_north = padded.shape[3] - 2
    extent_deep = padded.shape[4] - 2
    even_rows = padded[:, :, :, 1:extent_north + 1]
    odd_rows = 0.5 * (even_rows + padded[:, :, :, 2:extent_north + 2])
    widened = jnp.stack([even_rows, odd_rows], axis=4)
    widened = widened.reshape(widened.shape[:3] + (2 * extent_north, extent_deep + 2))
    even_layers = widened[..., 1:extent_deep + 1]
    odd_layers = 0.5 * (even_layers + widened[..., 2:extent_deep + 2])
    joined = jnp.stack([even_layers, odd_layers], axis=5)
    return joined.reshape(joined.shape[:4] + (2 * extent_deep,))


def factor_lines(below_diagonal, main_diagonal, above_diagonal, entering):
    def forward(factor_before, row_items):
        below_row, main_row, above_row = row_items
        pivots = main_row - below_row * factor_before
        factor = above_row / pivots
        return factor, (pivots, factor)

    ignored, (pivot_rows, factor_rows) = lax.scan(forward, entering, (jnp.moveaxis(below_diagonal, 1, 0), jnp.moveaxis(main_diagonal, 1, 0), jnp.moveaxis(above_diagonal, 1, 0)))
    return jnp.moveaxis(pivot_rows, 0, 1), jnp.moveaxis(factor_rows, 0, 1)


def eliminate_rows(source, below_diagonal, pivots):
    def forward(earlier_row, row_items):
        below_row, pivot_row, source_row = row_items
        eliminated = (source_row - spread(below_row) * earlier_row) / spread(pivot_row)
        return eliminated, eliminated

    ignored, rows_out = lax.scan(forward, jnp.zeros(source[:, :, 0].shape, jnp.float32), (jnp.moveaxis(below_diagonal, 1, 0), jnp.moveaxis(pivots, 1, 0), jnp.moveaxis(source, 2, 0)))
    return jnp.moveaxis(rows_out, 0, 2)


def substitute_rows(eliminated, factors):
    def backward(next_value, row_items):
        factor_row, reduced_row = row_items
        solved = reduced_row - spread(factor_row) * next_value
        return solved, solved

    ignored, rows_out = lax.scan(backward, jnp.zeros(eliminated[:, :, 0].shape, jnp.float32), (jnp.moveaxis(factors, 1, 0), jnp.moveaxis(eliminated, 2, 0)), reverse=True)
    return jnp.moveaxis(rows_out, 0, 2)


def line_solve(source, grid_level):
    below_diagonal = -grid_level[3]
    pivots, factors = factor_lines(below_diagonal, grid_level[6], -grid_level[0], jnp.zeros(grid_level[6][:, 0].shape, jnp.float32))
    return substitute_rows(eliminate_rows(source, below_diagonal, pivots), factors)


def cycle_reference(nodal_source, fine_level, coarse_level):
    smoothed = line_solve(nodal_source, fine_level)
    residue = nodal_source - apply_padded(pad_space(smoothed), fine_level)
    coarse_source = restrict_plane(pad_space(residue)[:, :, 1:-1])
    correction = line_solve(coarse_source, coarse_level)
    for repeat in range(COARSE_SWEEPS - 1):
        correction = line_solve(coarse_source + side_padded(pad_space(correction)[:, :, 1:-1], coarse_level), coarse_level)
    smoothed = smoothed + prolong_plane(pad_space(correction)[:, :, 1:-1])
    return line_solve(nodal_source + side_padded(pad_space(smoothed)[:, :, 1:-1], fine_level), fine_level)


def reference(residual, classes, edge_mask, class_weight):
    cell_values = class_weight[classes]
    free_edges = (1 - edge_mask).astype(jnp.float32)
    masses, edge_diagonal, kind_weights = edge_coefficients(cell_values, free_edges)
    fine_level = make_level(kind_weights)
    coarse_level = make_level(coarse_weights(kind_weights))
    source = residual * free_edges
    first = edge_damping * source / edge_diagonal * free_edges
    remainder = source - curl_apply(pad_space(first), masses) * free_edges
    rimmed = pad_space(remainder)
    nodal_source = jnp.concatenate([gradient_adjoint(rimmed), average_adjoint(rimmed)], axis=1)
    potential = cycle_reference(nodal_source, fine_level, coarse_level)
    rimmed = pad_space(potential)
    second = first + (gradient_edges(rimmed) + average_edges(rimmed)) * free_edges
    remainder = source - curl_apply(pad_space(second), masses) * free_edges
    return second + edge_damping * remainder / edge_diagonal * free_edges
```

```python
import jax
import jax.numpy as jnp
from jax import lax
from jax.experimental import pallas as pl
from jax.experimental.pallas import tpu as pltpu
from jax.sharding import PartitionSpec as P

aspect = 2.0
face_weight = (1.0 / (aspect * aspect), 1.0, 1.0)
mass_factor = (aspect * aspect, 1.0, 1.0)
stiff_weight = (
    2.0 * (face_weight[1] + face_weight[2]),
    2.0 * (face_weight[0] + face_weight[2]),
    2.0 * (face_weight[0] + face_weight[1]),
)
edge_damping = 0.6
shift_ratio = 0.0001
shift_added = 0.05
coarse_along = 0.5625
coarse_across = 0.1875


def extended(block, sides, width):
    for axis, dim in sides:
        count = lax.axis_size(axis)
        forward = [(i, i + 1) for i in range(count - 1)]
        backward = [(target, source) for source, target in forward]
        low = lax.ppermute(
            lax.slice_in_dim(block, block.shape[dim] - width, None, axis=dim), axis, forward
        )
        high = lax.ppermute(lax.slice_in_dim(block, 0, width, axis=dim), axis, backward)
        block = jnp.concatenate([low, block, high], axis=dim)
    return block


def shifted(values, axis_index):
    axis_index = axis_index % values.ndim
    length = values.shape[axis_index]
    widths = [(0, 0)] * values.ndim
    widths[axis_index] = (1, 0)
    return lax.slice_in_dim(jnp.pad(values, widths), 0, length, axis=axis_index)


def spread(per_kind):
    scalar_kind = per_kind[0:1]
    vector_kind = per_kind[1:2]
    return jnp.concatenate([scalar_kind, vector_kind, vector_kind, vector_kind], axis=0)


def edge_coefficients(cell_values, free_edges):
    cells_west = shifted(cell_values, 0)
    cells_south = shifted(cell_values, 1)
    cells_above = shifted(cell_values, 2)
    first_edges = 0.25 * (cell_values + cells_south + cells_above + shifted(cells_above, 1))
    second_edges = 0.25 * (cell_values + cells_west + cells_above + shifted(cells_above, 0))
    third_edges = 0.25 * (cell_values + cells_west + cells_south + shifted(cells_south, 0))
    averages = jnp.stack([first_edges, second_edges, third_edges])
    factors = jnp.array(mass_factor, jnp.float32).reshape(3, 1, 1, 1)
    stiffness = jnp.array(stiff_weight, jnp.float32).reshape(3, 1, 1, 1)
    masses = factors * averages * free_edges
    edge_diagonal = stiffness + masses
    kind_weights = jnp.stack([masses, edge_diagonal * free_edges])
    return (masses, edge_diagonal, kind_weights)


def coarse_weights(kind_weights):
    grouped = kind_weights.reshape(
        kind_weights.shape[:3] + (kind_weights.shape[3] // 2, 2, kind_weights.shape[4] // 2, 2)
    )
    summed = (
        grouped[:, :, :, :, 0, :, 0]
        + grouped[:, :, :, :, 1, :, 0]
        + (grouped[:, :, :, :, 0, :, 1] + grouped[:, :, :, :, 1, :, 1])
    )
    factors = jnp.array([coarse_along, coarse_across, coarse_across], jnp.float32).reshape(
        1, 3, 1, 1, 1
    )
    return summed * factors


def level_from(
    weights_pad, start_east, start_north, start_deep, extent_east, extent_north, extent_deep
):

    def window(component, back_east, back_north, back_deep):
        low_east = start_east - back_east
        low_north = start_north - back_north
        low_deep = start_deep - back_deep
        return weights_pad[
            :,
            component,
            low_east : low_east + extent_east,
            low_north : low_north + extent_north,
            low_deep : low_deep + extent_deep,
        ]

    to_east = window(0, 0, 0, 0)
    to_north = window(1, 0, 0, 0)
    to_deep = window(2, 0, 0, 0)
    to_west = window(0, 1, 0, 0)
    to_south = window(1, 0, 1, 0)
    to_shallow = window(2, 0, 0, 1)
    weight_sum = to_east + to_west + to_north + to_south + to_deep + to_shallow
    return (
        to_east,
        to_north,
        to_deep,
        to_west,
        to_south,
        to_shallow,
        (1.0 + shift_ratio) * weight_sum + shift_added,
    )


def curl_apply(padded, masses):
    extent_east = padded.shape[2] - 2
    extent_north = padded.shape[3] - 2
    extent_deep = padded.shape[4] - 2

    def region(values, move_east, move_north, move_deep, extra_cells):
        return values[
            :,
            move_east : move_east + extent_east + extra_cells,
            move_north : move_north + extent_north + extra_cells,
            move_deep : move_deep + extent_deep + extra_cells,
        ]

    field_east = padded[:, 0]
    field_north = padded[:, 1]
    field_deep = padded[:, 2]
    flux_east = face_weight[0] * (
        region(field_deep, 0, 1, 0, 1)
        - region(field_deep, 0, 0, 0, 1)
        - (region(field_north, 0, 0, 1, 1) - region(field_north, 0, 0, 0, 1))
    )
    flux_north = face_weight[1] * (
        region(field_east, 0, 0, 1, 1)
        - region(field_east, 0, 0, 0, 1)
        - (region(field_deep, 1, 0, 0, 1) - region(field_deep, 0, 0, 0, 1))
    )
    flux_deep = face_weight[2] * (
        region(field_north, 1, 0, 0, 1)
        - region(field_north, 0, 0, 0, 1)
        - (region(field_east, 0, 1, 0, 1) - region(field_east, 0, 0, 0, 1))
    )
    out_east = (
        region(flux_north, 1, 1, 0, 0)
        - region(flux_north, 1, 1, 1, 0)
        - (region(flux_deep, 1, 0, 1, 0) - region(flux_deep, 1, 1, 1, 0))
        + masses[0] * region(field_east, 1, 1, 1, 0)
    )
    out_north = (
        region(flux_deep, 0, 1, 1, 0)
        - region(flux_deep, 1, 1, 1, 0)
        - (region(flux_east, 1, 1, 0, 0) - region(flux_east, 1, 1, 1, 0))
        + masses[1] * region(field_north, 1, 1, 1, 0)
    )
    out_deep = (
        region(flux_east, 1, 0, 1, 0)
        - region(flux_east, 1, 1, 1, 0)
        - (region(flux_north, 0, 1, 1, 0) - region(flux_north, 1, 1, 1, 0))
        + masses[2] * region(field_deep, 1, 1, 1, 0)
    )
    return jnp.stack([out_east, out_north, out_deep], axis=1)


def side_padded(plane_pad, grid_level):
    return (
        spread(grid_level[1]) * plane_pad[..., 2:, 1:-1]
        + spread(grid_level[4]) * plane_pad[..., :-2, 1:-1]
        + spread(grid_level[2]) * plane_pad[..., 1:-1, 2:]
        + spread(grid_level[5]) * plane_pad[..., 1:-1, :-2]
    )


def apply_padded(padded, grid_level):
    center = padded[:, :, 1:-1, 1:-1, 1:-1]
    along_line = (
        spread(grid_level[0]) * padded[:, :, 2:, 1:-1, 1:-1]
        + spread(grid_level[3]) * padded[:, :, :-2, 1:-1, 1:-1]
    )
    return spread(grid_level[6]) * center - (
        along_line + side_padded(padded[:, :, 1:-1], grid_level)
    )


def gradient_adjoint(padded):
    interior = padded[:, :, 1:-1, 1:-1, 1:-1]
    from_west = padded[:, 0, :-2, 1:-1, 1:-1]
    from_south = padded[:, 1, 1:-1, :-2, 1:-1]
    from_above = padded[:, 2, 1:-1, 1:-1, :-2]
    total_flow = (
        from_west - interior[:, 0] + (from_south - interior[:, 1]) + (from_above - interior[:, 2])
    )
    return total_flow[:, None]


def average_adjoint(padded):
    interior = padded[:, :, 1:-1, 1:-1, 1:-1]
    return jnp.stack(
        [
            0.5 * (interior[:, 0] + padded[:, 0, :-2, 1:-1, 1:-1]),
            0.5 * (interior[:, 1] + padded[:, 1, 1:-1, :-2, 1:-1]),
            0.5 * (interior[:, 2] + padded[:, 2, 1:-1, 1:-1, :-2]),
        ],
        axis=1,
    )


def gradient_edges(padded):
    interior = padded[:, 0, 1:-1, 1:-1, 1:-1]
    return jnp.stack(
        [
            padded[:, 0, 2:, 1:-1, 1:-1] - interior,
            padded[:, 0, 1:-1, 2:, 1:-1] - interior,
            padded[:, 0, 1:-1, 1:-1, 2:] - interior,
        ],
        axis=1,
    )


def average_edges(padded):
    return jnp.stack(
        [
            0.5 * (padded[:, 1, 1:-1, 1:-1, 1:-1] + padded[:, 1, 2:, 1:-1, 1:-1]),
            0.5 * (padded[:, 2, 1:-1, 1:-1, 1:-1] + padded[:, 2, 1:-1, 2:, 1:-1]),
            0.5 * (padded[:, 3, 1:-1, 1:-1, 1:-1] + padded[:, 3, 1:-1, 1:-1, 2:]),
        ],
        axis=1,
    )


def restrict_plane(padded):
    extent_north = padded.shape[3] - 2
    extent_deep = padded.shape[4] - 2
    halved = padded[:, :, :, 1 : extent_north + 1 : 2] + 0.5 * (
        padded[:, :, :, 0:extent_north:2] + padded[:, :, :, 2 : extent_north + 2 : 2]
    )
    return halved[..., 1 : extent_deep + 1 : 2] + 0.5 * (
        halved[..., 0:extent_deep:2] + halved[..., 2 : extent_deep + 2 : 2]
    )


def prolong_plane(padded):
    extent_north = padded.shape[3] - 2
    extent_deep = padded.shape[4] - 2
    even_rows = padded[:, :, :, 1 : extent_north + 1]
    odd_rows = 0.5 * (even_rows + padded[:, :, :, 2 : extent_north + 2])
    widened = jnp.stack([even_rows, odd_rows], axis=4)
    widened = widened.reshape(widened.shape[:3] + (2 * extent_north, extent_deep + 2))
    even_layers = widened[..., 1 : extent_deep + 1]
    odd_layers = 0.5 * (even_layers + widened[..., 2 : extent_deep + 2])
    joined = jnp.stack([even_layers, odd_layers], axis=5)
    return joined.reshape(joined.shape[:4] + (2 * extent_deep,))


def factor_lines(below_diagonal, main_diagonal, above_diagonal, entering):

    def forward(factor_before, row_items):
        below_row, main_row, above_row = row_items
        pivots = main_row - below_row * factor_before
        factor = above_row / pivots
        return (factor, (pivots, factor))

    ignored, (pivot_rows, factor_rows) = lax.scan(
        forward,
        entering,
        (
            jnp.moveaxis(below_diagonal, 1, 0),
            jnp.moveaxis(main_diagonal, 1, 0),
            jnp.moveaxis(above_diagonal, 1, 0),
        ),
    )
    return (jnp.moveaxis(pivot_rows, 0, 1), jnp.moveaxis(factor_rows, 0, 1))


def eliminate_rows(source, below_diagonal, pivots):

    def forward(earlier_row, row_items):
        below_row, pivot_row, source_row = row_items
        eliminated = (source_row - spread(below_row) * earlier_row) / spread(pivot_row)
        return (eliminated, eliminated)

    ignored, rows_out = lax.scan(
        forward,
        jnp.zeros(source[:, :, 0].shape, jnp.float32),
        (
            jnp.moveaxis(below_diagonal, 1, 0),
            jnp.moveaxis(pivots, 1, 0),
            jnp.moveaxis(source, 2, 0),
        ),
    )
    return jnp.moveaxis(rows_out, 0, 2)


def substitute_rows(eliminated, factors):

    def backward(next_value, row_items):
        factor_row, reduced_row = row_items
        solved = reduced_row - spread(factor_row) * next_value
        return (solved, solved)

    ignored, rows_out = lax.scan(
        backward,
        jnp.zeros(eliminated[:, :, 0].shape, jnp.float32),
        (jnp.moveaxis(factors, 1, 0), jnp.moveaxis(eliminated, 2, 0)),
        reverse=True,
    )
    return jnp.moveaxis(rows_out, 0, 2)


def plain_solve(right_side, below_diagonal, pivots, factors):

    def forward(earlier_row, row_items):
        below_row, pivot_row, source_row = row_items
        eliminated = (source_row - below_row * earlier_row) / pivot_row
        return (eliminated, eliminated)

    ignored, rows_out = lax.scan(
        forward,
        jnp.zeros(right_side[:, 0].shape, jnp.float32),
        (
            jnp.moveaxis(below_diagonal, 1, 0),
            jnp.moveaxis(pivots, 1, 0),
            jnp.moveaxis(right_side, 1, 0),
        ),
    )

    def backward(next_value, row_items):
        factor_row, reduced_row = row_items
        solved = reduced_row - factor_row * next_value
        return (solved, solved)

    ignored, solved_rows = lax.scan(
        backward,
        jnp.zeros(right_side[:, 0].shape, jnp.float32),
        (jnp.moveaxis(factors, 1, 0), rows_out),
        reverse=True,
    )
    return jnp.moveaxis(solved_rows, 0, 1)


def spike_level(grid_level):
    below_diagonal = -grid_level[3]
    main_diagonal = grid_level[6]
    above_diagonal = -grid_level[0]
    pivots, factors = factor_lines(
        below_diagonal,
        main_diagonal,
        above_diagonal,
        jnp.zeros(main_diagonal[:, 0].shape, jnp.float32),
    )
    inner_zero = jnp.zeros_like(main_diagonal[:, 1:])
    spike_before = plain_solve(
        jnp.concatenate([below_diagonal[:, :1], inner_zero], axis=1),
        below_diagonal,
        pivots,
        factors,
    )
    spike_after = plain_solve(
        jnp.concatenate([inner_zero, above_diagonal[:, -1:]], axis=1),
        below_diagonal,
        pivots,
        factors,
    )
    end_rows = jnp.stack(
        [spike_before[:, 0], spike_before[:, -1], spike_after[:, 0], spike_after[:, -1]], axis=1
    )
    return (
        (below_diagonal, pivots, factors, spike_before, spike_after),
        end_rows.reshape(end_rows.shape[:2] + (1, -1)),
    )


def reduce_chain(coefficients):
    before_first, before_last, after_first, after_last = (
        coefficients[:, member] for member in range(4)
    )

    def forward(beta_before, row_items):
        first_row, last_row, next_first, next_last = row_items
        denominator = 1.0 - first_row * beta_before
        scaled = next_first / denominator
        beta_after = next_last + last_row * beta_before * scaled
        return (beta_after, (denominator, scaled, beta_before, beta_after))

    ignored, outputs = lax.scan(
        forward,
        jnp.zeros(before_first[:, 0].shape, jnp.float32),
        tuple(
            (
                jnp.moveaxis(values, 1, 0)
                for values in (before_first, before_last, after_first, after_last)
            )
        ),
    )
    denominators, scaled_rows, betas_before, betas_after = (
        jnp.moveaxis(values, 0, 1) for values in outputs
    )
    return (before_first, before_last, denominators, scaled_rows, betas_before, betas_after)


def reduced_factors(fine_level, coarse_level):
    fine_data, fine_ends = spike_level(fine_level)
    coarse_data, coarse_ends = spike_level(coarse_level)
    fine_rows, coarse_rows = (
        lax.all_to_all(fine_ends, "gx", split_axis=3, concat_axis=2, tiled=True),
        lax.all_to_all(coarse_ends, "gx", split_axis=3, concat_axis=2, tiled=True),
    )
    return (fine_data + (reduce_chain(fine_rows),), coarse_data + (reduce_chain(coarse_rows),))


def reduced_solve(source, line_data):
    below_diagonal, pivots, factors, spike_before, spike_after, reduced = line_data
    local_rows = substitute_rows(eliminate_rows(source, below_diagonal, pivots), factors)
    end_values = jnp.stack([local_rows[:, :, 0], local_rows[:, :, -1]], axis=2)
    end_values = end_values.reshape(end_values.shape[:3] + (-1,))
    spread_rows = tuple((jnp.moveaxis(spread(values), 1, 0) for values in reduced))
    exchanged = lax.all_to_all(end_values, "gx", split_axis=3, concat_axis=2, tiled=True)
    paired = exchanged.reshape(
        exchanged.shape[:2] + (exchanged.shape[2] // 2, 2, exchanged.shape[3])
    )
    first_values = jnp.moveaxis(paired[:, :, :, 0], 2, 0)
    last_values = jnp.moveaxis(paired[:, :, :, 1], 2, 0)
    before_first, before_last, denominators, scaled_rows, betas_before, betas_after = spread_rows

    def forward(carried, row_items):
        first_row, last_row, couple_first, couple_last, denominator, beta_before = row_items
        leading = (first_row - couple_first * carried) / denominator
        trailing = last_row - couple_last * (carried - beta_before * leading)
        return (trailing, (leading, trailing))

    ignored, (leading_rows, trailing_rows) = lax.scan(
        forward,
        jnp.zeros(first_values[0].shape, jnp.float32),
        (first_values, last_values, before_first, before_last, denominators, betas_before),
    )

    def backward(next_first, row_items):
        leading, trailing, scaled, beta_after = row_items
        solved_first = leading - scaled * next_first
        solved_last = trailing - beta_after * next_first
        return (solved_first, (next_first, solved_last))

    ignored, (next_firsts, solved_lasts) = lax.scan(
        backward,
        jnp.zeros(first_values[0].shape, jnp.float32),
        (leading_rows, trailing_rows, scaled_rows, betas_after),
        reverse=True,
    )
    previous_lasts = jnp.concatenate([jnp.zeros_like(solved_lasts[:1]), solved_lasts[:-1]], axis=0)
    coupled = jnp.stack([previous_lasts, next_firsts], axis=1)
    coupled = jnp.moveaxis(coupled.reshape((-1,) + coupled.shape[2:]), 0, 2)
    couplings = lax.all_to_all(coupled, "gx", split_axis=2, concat_axis=3, tiled=True)
    couplings = couplings.reshape(couplings.shape[:3] + local_rows.shape[3:])
    return (
        local_rows
        - spread(spike_before) * couplings[:, :, 0:1]
        - spread(spike_after) * couplings[:, :, 1:2]
    )


def line_relax(source, line_data):
    return reduced_solve(source, line_data)


def edge_rims(values, rim_width):
    return extended(values, (("gx", 2), ("gy", 3), ("gz", 4)), rim_width)


def node_rims(values):
    return extended(values, (("gx", 2), ("gy", 3), ("gz", 4)), 1)


def coarse_plane(values):
    return node_rims(values)[:, :, 1:-1]


def cycle_body(nodal_source, fine_level, coarse_level, fine_lines, coarse_lines):
    smoothed = line_relax(nodal_source, fine_lines)
    residue = nodal_source - apply_padded(node_rims(smoothed), fine_level)
    coarse_source = restrict_plane(node_rims(residue)[:, :, 1:-1])
    correction = line_relax(coarse_source, coarse_lines)
    correction = line_relax(
        coarse_source + side_padded(coarse_plane(correction), coarse_level), coarse_lines
    )
    widened = coarse_plane(correction)
    smoothed = smoothed + prolong_plane(widened)
    return line_relax(
        nodal_source + side_padded(node_rims(smoothed)[:, :, 1:-1], fine_level), fine_lines
    )


def per_device_permutes(residual, classes, edge_mask, class_weight):
    labels = jnp.arange(class_weight.shape[0], dtype=jnp.int32).reshape(-1, 1, 1, 1)
    cell_values = jnp.sum(
        jnp.where(classes[None] == labels, class_weight.reshape(-1, 1, 1, 1), 0.0), axis=0
    )
    free_edges = (1 - edge_mask).astype(jnp.float32)
    material = jnp.concatenate([cell_values[None], free_edges], axis=0)[None]
    material_pad = edge_rims(material, 2)[0]
    masses_pad, diagonal_pad, kinds_pad = edge_coefficients(material_pad[0], material_pad[1:])
    masses = masses_pad[:, 2:-2, 2:-2, 2:-2]
    edge_diagonal = diagonal_pad[:, 2:-2, 2:-2, 2:-2]
    extent_east = residual.shape[2]
    extent_north = residual.shape[3]
    extent_deep = residual.shape[4]
    fine_level = level_from(kinds_pad, 2, 2, 2, extent_east, extent_north, extent_deep)
    coarse_level = level_from(
        coarse_weights(kinds_pad), 2, 1, 1, extent_east, extent_north // 2, extent_deep // 2
    )
    fine_lines, coarse_lines = reduced_factors(fine_level, coarse_level)
    source = residual * free_edges
    first = edge_damping * source / edge_diagonal * free_edges
    remainder = source - curl_apply(edge_rims(first, 1), masses) * free_edges
    rimmed = node_rims(remainder)
    nodal_source = jnp.concatenate([gradient_adjoint(rimmed), average_adjoint(rimmed)], axis=1)
    potential = cycle_body(nodal_source, fine_level, coarse_level, fine_lines, coarse_lines)
    rimmed = node_rims(potential)
    second = first + (gradient_edges(rimmed) + average_edges(rimmed)) * free_edges
    remainder = source - curl_apply(edge_rims(second, 1), masses) * free_edges
    return second + edge_damping * remainder / edge_diagonal * free_edges


def split_dot(left, right):
    high = left.astype(jnp.bfloat16)
    low = (left - high.astype(jnp.float32)).astype(jnp.bfloat16)
    return jnp.dot(high, right, preferred_element_type=jnp.float32) + jnp.dot(
        low, right, preferred_element_type=jnp.float32
    )


def dot_split(left, right):
    high = right.astype(jnp.bfloat16)
    low = (right - high.astype(jnp.float32)).astype(jnp.bfloat16)
    return jnp.dot(left, high, preferred_element_type=jnp.float32) + jnp.dot(
        left, low, preferred_element_type=jnp.float32
    )


def gather_kernel(
    counts, residual, classes, edge_mask, class_weight, out,
    data, mass, stiff, damp, field, nodal, sides, diagonal, inverse, east_scaled, west_scaled,
    potential, residue, coarse_weight, coarse_sides, coarse_inverse, coarse_east, coarse_west,
    coarse_source, correction, second, result, arrived,
    send_z, recv_z, send_x, recv_x, send_c, recv_c, send_out, recv_out,
):
    ngx, ngy, ngz = counts
    gx, gy, gz = (lax.axis_index(name) for name in ("gx", "gy", "gz"))
    xb, yb, zb = classes.shape
    nx, ny, nz = xb * ngx, yb * ngy, zb * ngz
    yc, zc = ny // 2, nz // 2

    barrier = pltpu.get_barrier_semaphore()
    peers = (
        [{"gx": lax.rem(gx + step, ngx)} for step in range(1, ngx)]
        + [{"gy": lax.rem(gy + step, ngy)} for step in range(1, ngy)]
        + [{"gz": lax.rem(gz + step, ngz)} for step in range(1, ngz)]
    )
    for peer in peers:
        pl.semaphore_signal(barrier, inc=1, device_id=peer, device_id_type=pl.DeviceIdType.MESH)

    def block(low, size, bx, by, bz):
        return data.at[
            pl.ds(low, size),
            pl.ds(bx * xb + 1, xb),
            pl.ds(pl.multiple_of(by * yb, 8), yb),
            pl.ds(pl.multiple_of(bz * zb, 128), zb),
        ]

    own = block(0, 10, gx, gy, gz)
    labels = classes[...]
    cells = jnp.full(labels.shape, class_weight[0], jnp.float32)
    for label in range(1, class_weight.shape[0]):
        cells = jnp.where(labels == label, class_weight[label], cells)
    own[0:3] = residual[0]
    own[3] = cells
    own[4:7] = (1 - edge_mask[...]).astype(jnp.float32)
    own[7:10] = residual[1]

    pl.semaphore_wait(barrier, len(peers))

    sends = []

    def send(source, target_peer, send_sem, recv_sem):
        copy = pltpu.make_async_remote_copy(
            src_ref=source, dst_ref=source, send_sem=send_sem, recv_sem=recv_sem,
            device_id=target_peer, device_id_type=pl.DeviceIdType.MESH,
        )
        copy.start()
        sends.append(copy)

    def arrival(ref, sem_send, sem_recv, peer):
        pltpu.make_async_remote_copy(
            src_ref=ref, dst_ref=ref, send_sem=sem_send, recv_sem=sem_recv,
            device_id=peer, device_id_type=pl.DeviceIdType.MESH,
        ).wait_recv()

    steps = sorted(range(1, ngx), key=lambda step: min(step, ngx - step))

    def to_cores(ky, k, bx, by):
        for kz in range(1, ngz):
            other = lax.rem(gz + ngz - kz, ngz)
            send(block(3 * other, 7, bx, by, gz), {"gz": other}, send_c.at[kz - 1, ky, k], recv_c.at[kz - 1, ky, k])

    def to_rows(k, bx):
        for ky in range(1, ngy):
            send(block(0, 10, bx, gy, gz), {"gy": lax.rem(gy + ngy - ky, ngy)}, send_x.at[ky - 1, k], recv_x.at[ky - 1, k])

    for k in steps:
        send(own, {"gx": lax.rem(gx + ngx - k, ngx)}, send_z.at[k], recv_z.at[k])
    to_rows(0, gx)
    to_cores(0, 0, gx, gy)

    zero_plane = jnp.zeros((ny, nz), jnp.float32)
    for member in range(3, 7):
        data[member, 0] = zero_plane
        data[member, nx + 1] = zero_plane
    for member in range(3):
        field[member, 0] = zero_plane
        field[member, nx + 1] = zero_plane
    for member in range(4):
        for plane in (0, nx + 1, nx + 2):
            potential[member, plane] = zero_plane

    for k in steps:
        bx = lax.rem(gx + k, ngx)
        arrival(block(0, 10, bx, gy, gz), send_z.at[k], recv_z.at[k], {"gx": bx})
        to_rows(k, bx)
        to_cores(0, k, bx, gy)
    for ky in range(1, ngy):
        by = lax.rem(gy + ky, ngy)
        for k in [0] + steps:
            bx = lax.rem(gx + k, ngx)
            arrival(block(0, 10, bx, by, gz), send_x.at[ky - 1, k], recv_x.at[ky - 1, k], {"gy": by})
            to_cores(ky, k, bx, by)
    for kz in range(1, ngz):
        bz = lax.rem(gz + kz, ngz)
        for ky in range(ngy):
            by = lax.rem(gy + ky, ngy)
            for k in [0] + steps:
                bx = lax.rem(gx + k, ngx)
                arrival(block(3 * gz, 7, bx, by, bz), send_c.at[kz - 1, ky, k], recv_c.at[kz - 1, ky, k], {"gz": bz})
    for copy in sends:
        copy.wait_send()

    mine = 7 * gz

    def edges_of(rows, layers):
        at_row = lax.broadcasted_iota(jnp.int32, (rows, layers), 0)
        at_layer = lax.broadcasted_iota(jnp.int32, (rows, layers), 1)
        masks = (at_row == 0, at_row == rows - 1, at_layer == 0, at_layer == layers - 1)

        def y_low(v):
            return jnp.where(masks[0], 0.0, pltpu.roll(v, 1, 0))

        def y_high(v):
            return jnp.where(masks[1], 0.0, pltpu.roll(v, rows - 1, 0))

        def z_low(v):
            return jnp.where(masks[2], 0.0, pltpu.roll(v, 1, 1))

        def z_high(v):
            return jnp.where(masks[3], 0.0, pltpu.roll(v, layers - 1, 1))

        return masks, y_low, y_high, z_low, z_high

    masks, y_low, y_high, z_low, z_high = edges_of(ny, nz)
    _, cy_low, cy_high, cz_low, cz_high = edges_of(yc, zc)

    def level_plane(kind, i, w1, w2, w3, carry, low_y, low_z, sides_ref, inverse_ref, east_ref, west_ref):
        west, east_before = carry
        south = low_y(w2)
        shallow = low_z(w3)
        main = (1.0 + shift_ratio) * (((((w1 + west) + w2) + south) + w3) + shallow) + shift_added
        q = 1.0 / (main - west * east_before)
        east = w1 * q
        sides_ref[kind, 0, i] = w2
        sides_ref[kind, 1, i] = south
        sides_ref[kind, 2, i] = w3
        sides_ref[kind, 3, i] = shallow
        inverse_ref[kind, i] = q
        east_ref[kind, i] = east
        west_ref[kind, i] = west * q
        return (w1, east)

    def materials(i, carry):
        c0 = data[3, i + 1]
        west = data[3, i]
        above = z_low(c0)
        south = y_low(c0)
        both = c0 + west
        averages = (
            0.25 * (((c0 + south) + above) + y_low(above)),
            0.25 * ((both + above) + z_low(west)),
            0.25 * ((both + south) + y_low(west)),
        )
        masses, strong = [], []
        for d in range(3):
            free = data[4 + d, i + 1]
            m = mass_factor[d] * averages[d] * free
            diag = stiff_weight[d] + m
            k = edge_damping * free / diag
            masses.append(m)
            strong.append(diag * free)
            mass[d, i] = m
            stiff[d, i] = strong[d]
            damp[d, i] = k
            field[d, i + 1] = data[mine + d, i + 1] * k
        return (
            level_plane(0, i, *masses, carry[0], y_low, z_low, sides, inverse, east_scaled, west_scaled),
            level_plane(1, i, *strong, carry[1], y_low, z_low, sides, inverse, east_scaled, west_scaled),
        )

    lax.fori_loop(0, nx, materials, ((zero_plane, zero_plane), (zero_plane, zero_plane)))

    def mat(shape, fn):
        return jnp.where(
            fn(lax.broadcasted_iota(jnp.int32, shape, 0), lax.broadcasted_iota(jnp.int32, shape, 1)), 1.0, 0.0
        )

    sum_z = mat((nz, zc), lambda r, c: r // 2 == c).astype(jnp.bfloat16)
    sum_y = mat((nx * yc, nx * ny), lambda r, c: r == c // 2).astype(jnp.bfloat16)
    rest_z = (
        mat((nz, zc), lambda r, c: r == 2 * c)
        + 0.5 * mat((nz, zc), lambda r, c: (r == 2 * c + 1) | (r == 2 * c - 1))
    ).astype(jnp.bfloat16)
    rest_y = (
        mat((nx * yc, nx * ny), lambda r, c: c == 2 * r)
        + 0.5 * mat(
            (nx * yc, nx * ny),
            lambda r, c: (c == 2 * r + 1) | ((c == 2 * r - 1) & (lax.rem(r, yc) != 0)),
        )
    ).astype(jnp.bfloat16)
    prol_z = (
        mat((zc, nz), lambda r, c: c == 2 * r)
        + 0.5 * mat((zc, nz), lambda r, c: (c == 2 * r + 1) | (c == 2 * r - 1))
    ).astype(jnp.bfloat16)
    prol_y = (
        mat((nx * ny, nx * yc), lambda r, c: r == 2 * c)
        + 0.5 * mat(
            (nx * ny, nx * yc),
            lambda r, c: (r == 2 * c + 1) | ((r == 2 * c - 1) & (lax.rem(c, yc) != 0)),
        )
    ).astype(jnp.bfloat16)

    for kind, weights in enumerate((mass, stiff)):
        for d in range(3):
            summed = dot_split(sum_y, split_dot(weights[d].reshape(nx * ny, nz), sum_z))
            factor = coarse_along if d == 0 else coarse_across
            coarse_weight[kind, d] = (factor * summed).reshape(nx, yc, zc)

    def coarse_level(i, carry):
        return tuple(
            level_plane(
                kind, i, coarse_weight[kind, 0, i], coarse_weight[kind, 1, i], coarse_weight[kind, 2, i],
                carry[kind], cy_low, cz_low, coarse_sides, coarse_inverse, coarse_east, coarse_west,
            )
            for kind in range(2)
        )

    coarse_zero = jnp.zeros((yc, zc), jnp.float32)
    lax.fori_loop(0, nx, coarse_level, ((coarse_zero, coarse_zero), (coarse_zero, coarse_zero)))

    def curl_plane(e, m, before):
        (e1, e2, e3), (next2, next3), (b2_before, b3_before) = e, m[0], before
        b1 = face_weight[0] * ((y_high(e3) - e3) - (z_high(e2) - e2))
        b2 = face_weight[1] * ((z_high(e1) - e1) - (next3 - e3))
        b3 = face_weight[2] * ((next2 - e2) - (y_high(e1) - e1))
        b1_y = jnp.where(masks[0], face_weight[0] * e3, pltpu.roll(b1, 1, 0))
        b1_z = jnp.where(masks[2], -face_weight[0] * e2, pltpu.roll(b1, 1, 1))
        b2_z = jnp.where(masks[2], face_weight[1] * e1, pltpu.roll(b2, 1, 1))
        b3_y = jnp.where(masks[0], -face_weight[2] * e1, pltpu.roll(b3, 1, 0))
        m1, m2, m3 = m[1]
        a1 = ((b2_z - b2) - (b3_y - b3)) + m1 * e1
        a2 = ((b3_before - b3) - (b1_z - b1)) + m2 * e2
        a3 = ((b1_y - b1) - (b2_before - b2)) + m3 * e3
        return (a1, a2, a3), (b2, b3)

    def faces_before(e1, e2, e3, next2, next3):
        b2 = face_weight[1] * ((z_high(e1) - e1) - (next3 - e3))
        b3 = face_weight[2] * ((next2 - e2) - (y_high(e1) - e1))
        return (b2, b3)

    def front(i, carry):
        before, rem1_before = carry
        e = tuple(field[d, i + 1] for d in range(3))
        applied, faces = curl_plane(
            e, ((field[1, i + 2], field[2, i + 2]), tuple(mass[d, i] for d in range(3))), before
        )
        r1, r2, r3 = (
            (data[mine + d, i + 1] - applied[d]) * data[4 + d, i + 1] for d in range(3)
        )
        r2_low = y_low(r2)
        r3_low = z_low(r3)
        nodal[0, i] = ((rem1_before - r1) + (r2_low - r2)) + (r3_low - r3)
        nodal[1, i] = 0.5 * (r1 + rem1_before)
        nodal[2, i] = 0.5 * (r2 + r2_low)
        nodal[3, i] = 0.5 * (r3 + r3_low)
        return (faces, r1)

    lax.fori_loop(
        0, nx, front,
        (faces_before(zero_plane, zero_plane, zero_plane, field[1, 1], field[2, 1]), zero_plane),
    )

    def side_sum(refs, kind, i, v, shifts):
        low_y, high_y, low_z, high_z = shifts
        return ((refs[kind, 0, i] * high_y(v) + refs[kind, 1, i] * low_y(v)) + refs[kind, 2, i] * high_z(v)) + refs[
            kind, 3, i
        ] * low_z(v)

    fine_shifts = (y_low, y_high, z_low, z_high)
    coarse_shifts = (cy_low, cy_high, cz_low, cz_high)

    def forward(i, carry):
        done = []
        for member in range(4):
            kind = min(member, 1)
            v = nodal[member, i] * inverse[kind, i] + west_scaled[kind, i] * carry[member]
            potential[member, i + 1] = v
            done.append(v)
        return tuple(done)

    def backward_residue(step, carry):
        i = nx - 1 - step
        done = []
        for member in range(4):
            kind = min(member, 1)
            v = potential[member, i + 1] + east_scaled[kind, i] * carry[member]
            potential[member, i + 1] = v
            residue[member, i] = side_sum(sides, kind, i, v, fine_shifts)
            done.append(v)
        return tuple(done)

    zeros4 = (zero_plane,) * 4
    lax.fori_loop(0, nx, forward, zeros4)
    lax.fori_loop(0, nx, backward_residue, zeros4)

    for member in range(4):
        coarse_source[member] = dot_split(
            rest_y, split_dot(residue[member].reshape(nx * ny, nz), rest_z)
        ).reshape(nx, yc, zc)

    def coarse_solve(first_time):
        def ahead(i, carry):
            done = []
            for member in range(4):
                kind = min(member, 1)
                b = coarse_source[member, i]
                if not first_time:
                    b = b + side_sum(coarse_sides, kind, i, correction[member, i], coarse_shifts)
                v = b * coarse_inverse[kind, i] + coarse_west[kind, i] * carry[member]
                correction[member, i] = v
                done.append(v)
            return tuple(done)

        def back(step, carry):
            i = nx - 1 - step
            done = []
            for member in range(4):
                v = correction[member, i] + coarse_east[min(member, 1), i] * carry[member]
                correction[member, i] = v
                done.append(v)
            return tuple(done)

        lax.fori_loop(0, nx, ahead, (coarse_zero,) * 4)
        lax.fori_loop(0, nx, back, (coarse_zero,) * 4)

    coarse_solve(True)
    for repeat in range(1):
        coarse_solve(False)

    for member in range(4):
        residue[member] = split_dot(
            dot_split(prol_y, correction[member].reshape(nx * yc, zc)), prol_z
        ).reshape(nx, ny, nz)

    def forward_again(i, carry):
        done = []
        for member in range(4):
            kind = min(member, 1)
            smoothed = potential[member, i + 1] + residue[member, i]
            b = nodal[member, i] + side_sum(sides, kind, i, smoothed, fine_shifts)
            v = b * inverse[kind, i] + west_scaled[kind, i] * carry[member]
            potential[member, i + 1] = v
            done.append(v)
        return tuple(done)

    def backward(step, carry):
        i = nx - 1 - step
        done = []
        for member in range(4):
            v = potential[member, i + 1] + east_scaled[min(member, 1), i] * carry[member]
            potential[member, i + 1] = v
            done.append(v)
        return tuple(done)

    lax.fori_loop(0, nx, forward_again, zeros4)
    lax.fori_loop(0, nx, backward, zeros4)

    base = gx * xb

    def update(step, carry):
        at = base + step
        p0, p1, p2, p3 = (potential[member, at] for member in range(4))
        second[0, step] = field[0, at] + ((potential[0, at + 1] - p0) + 0.5 * (p1 + potential[1, at + 1])) * data[4, at]
        second[1, step] = field[1, at] + ((y_high(p0) - p0) + 0.5 * (p2 + y_high(p2))) * data[5, at]
        second[2, step] = field[2, at] + ((z_high(p0) - p0) + 0.5 * (p3 + z_high(p3))) * data[6, at]
        return carry

    lax.fori_loop(0, xb + 2, update, 0)

    def finish(i, before):
        e = tuple(second[d, i + 1] for d in range(3))
        at = base + i
        applied, faces = curl_plane(
            e, ((second[1, i + 2], second[2, i + 2]), tuple(mass[d, at] for d in range(3))), before
        )
        for d in range(3):
            result[d, i] = e[d] + damp[d, at] * (data[mine + d, at + 1] - applied[d])
        return faces

    lax.fori_loop(
        0, xb, finish,
        faces_before(second[0, 0], second[1, 0], second[2, 0], second[1, 1], second[2, 1]),
    )

    def part(bz):
        return result.at[:, :, pl.ds(pl.multiple_of(gy * yb, 8), yb), pl.ds(pl.multiple_of(bz * zb, 128), zb)]

    other = 1 - gz
    swap = pltpu.make_async_remote_copy(
        src_ref=part(other), dst_ref=arrived, send_sem=send_out, recv_sem=recv_out,
        device_id={"gz": other}, device_id_type=pl.DeviceIdType.MESH,
    )
    swap.start()
    out[pl.ds(gz, 1)] = part(gz)[...][None]
    swap.wait()
    out[pl.ds(other, 1)] = arrived[...][None]


def per_device(residual, classes, edge_mask, class_weight):
    counts = tuple(lax.axis_size(name) for name in ("gx", "gy", "gz"))
    ngx, ngy, ngz = counts
    xb, yb, zb = classes.shape
    nx, ny, nz = xb * ngx, yb * ngy, zb * ngz
    cells = nx * ny * nz
    aligned = yb % 8 == 0 and zb % 128 == 0 and (ny // 2) % 8 == 0 and (nz // 2) % 128 == 0
    if ngz != 2 or residual.shape[0] != 2 or not aligned or cells * 4 * 80 > 48 * 2**20:
        return per_device_permutes(residual, classes, edge_mask, class_weight)
    yc, zc = ny // 2, nz // 2

    def held(*shape):
        return pltpu.VMEM(shape, jnp.float32)

    dma = pltpu.SemaphoreType.DMA
    vmem = pl.BlockSpec(memory_space=pltpu.VMEM)
    return pl.pallas_call(
        lambda *refs: gather_kernel(counts, *refs),
        out_shape=jax.ShapeDtypeStruct(residual.shape, jnp.float32),
        in_specs=[vmem, vmem, vmem, pl.BlockSpec(memory_space=pltpu.SMEM)],
        out_specs=vmem,
        scratch_shapes=[
            held(10, nx + 2, ny, nz),
            held(3, nx, ny, nz),
            held(3, nx, ny, nz),
            held(3, nx, ny, nz),
            held(3, nx + 2, ny, nz),
            held(4, nx, ny, nz),
            held(2, 4, nx, ny, nz),
            held(1, 1, 8, 128),
            held(2, nx, ny, nz),
            held(2, nx, ny, nz),
            held(2, nx, ny, nz),
            held(4, nx + 3, ny, nz),
            held(4, nx, ny, nz),
            held(2, 3, nx, yc, zc),
            held(2, 4, nx, yc, zc),
            held(2, nx, yc, zc),
            held(2, nx, yc, zc),
            held(2, nx, yc, zc),
            held(4, nx, yc, zc),
            held(4, nx, yc, zc),
            held(3, xb + 2, ny, nz),
            held(3, xb, ny, nz),
            held(3, xb, yb, zb),
            dma((ngx,)), dma((ngx,)),
            dma((max(ngy - 1, 1), ngx)), dma((max(ngy - 1, 1), ngx)),
            dma((ngz - 1, ngy, ngx)), dma((ngz - 1, ngy, ngx)),
            dma, dma,
        ],
        compiler_params=pltpu.CompilerParams(
            collective_id=0, has_side_effects=True, vmem_limit_bytes=60 * 2**20
        ),
    )(residual, classes, edge_mask, class_weight)


def solution(mesh):
    return jax.shard_map(
        per_device,
        mesh=mesh,
        in_specs=(
            P("period", None, "gx", "gy", "gz"),
            P("gx", "gy", "gz"),
            P(None, "gx", "gy", "gz"),
            P("period"),
        ),
        out_specs=P("period", None, "gx", "gy", "gz"),
        check_vma=False,
    )
```

```python
import jax
import jax.numpy as jnp
from jax import lax
from jax.experimental import pallas as pl
from jax.experimental.pallas import tpu as pltpu
from jax.sharding import PartitionSpec as P

aspect = 2.0
face_weight = (1.0 / (aspect * aspect), 1.0, 1.0)
mass_factor = (aspect * aspect, 1.0, 1.0)
stiff_weight = (
    2.0 * (face_weight[1] + face_weight[2]),
    2.0 * (face_weight[0] + face_weight[2]),
    2.0 * (face_weight[0] + face_weight[1]),
)
edge_damping = 0.6
shift_ratio = 0.0001
shift_added = 0.05
coarse_along = 0.5625
coarse_across = 0.1875


def extended(block, sides, width):
    for axis, dim in sides:
        count = lax.axis_size(axis)
        forward = [(i, i + 1) for i in range(count - 1)]
        backward = [(target, source) for source, target in forward]
        low = lax.ppermute(
            lax.slice_in_dim(block, block.shape[dim] - width, None, axis=dim), axis, forward
        )
        high = lax.ppermute(lax.slice_in_dim(block, 0, width, axis=dim), axis, backward)
        block = jnp.concatenate([low, block, high], axis=dim)
    return block


def shifted(values, axis_index):
    axis_index = axis_index % values.ndim
    length = values.shape[axis_index]
    widths = [(0, 0)] * values.ndim
    widths[axis_index] = (1, 0)
    return lax.slice_in_dim(jnp.pad(values, widths), 0, length, axis=axis_index)


def spread(per_kind):
    scalar_kind = per_kind[0:1]
    vector_kind = per_kind[1:2]
    return jnp.concatenate([scalar_kind, vector_kind, vector_kind, vector_kind], axis=0)


def edge_coefficients(cell_values, free_edges):
    cells_west = shifted(cell_values, 0)
    cells_south = shifted(cell_values, 1)
    cells_above = shifted(cell_values, 2)
    first_edges = 0.25 * (cell_values + cells_south + cells_above + shifted(cells_above, 1))
    second_edges = 0.25 * (cell_values + cells_west + cells_above + shifted(cells_above, 0))
    third_edges = 0.25 * (cell_values + cells_west + cells_south + shifted(cells_south, 0))
    averages = jnp.stack([first_edges, second_edges, third_edges])
    factors = jnp.array(mass_factor, jnp.float32).reshape(3, 1, 1, 1)
    stiffness = jnp.array(stiff_weight, jnp.float32).reshape(3, 1, 1, 1)
    masses = factors * averages * free_edges
    edge_diagonal = stiffness + masses
    kind_weights = jnp.stack([masses, edge_diagonal * free_edges])
    return (masses, edge_diagonal, kind_weights)


def coarse_weights(kind_weights):
    grouped = kind_weights.reshape(
        kind_weights.shape[:3] + (kind_weights.shape[3] // 2, 2, kind_weights.shape[4] // 2, 2)
    )
    summed = (
        grouped[:, :, :, :, 0, :, 0]
        + grouped[:, :, :, :, 1, :, 0]
        + (grouped[:, :, :, :, 0, :, 1] + grouped[:, :, :, :, 1, :, 1])
    )
    factors = jnp.array([coarse_along, coarse_across, coarse_across], jnp.float32).reshape(
        1, 3, 1, 1, 1
    )
    return summed * factors


def level_from(
    weights_pad, start_east, start_north, start_deep, extent_east, extent_north, extent_deep
):

    def window(component, back_east, back_north, back_deep):
        low_east = start_east - back_east
        low_north = start_north - back_north
        low_deep = start_deep - back_deep
        return weights_pad[
            :,
            component,
            low_east : low_east + extent_east,
            low_north : low_north + extent_north,
            low_deep : low_deep + extent_deep,
        ]

    to_east = window(0, 0, 0, 0)
    to_north = window(1, 0, 0, 0)
    to_deep = window(2, 0, 0, 0)
    to_west = window(0, 1, 0, 0)
    to_south = window(1, 0, 1, 0)
    to_shallow = window(2, 0, 0, 1)
    weight_sum = to_east + to_west + to_north + to_south + to_deep + to_shallow
    return (
        to_east,
        to_north,
        to_deep,
        to_west,
        to_south,
        to_shallow,
        (1.0 + shift_ratio) * weight_sum + shift_added,
    )


def curl_apply(padded, masses):
    extent_east = padded.shape[2] - 2
    extent_north = padded.shape[3] - 2
    extent_deep = padded.shape[4] - 2

    def region(values, move_east, move_north, move_deep, extra_cells):
        return values[
            :,
            move_east : move_east + extent_east + extra_cells,
            move_north : move_north + extent_north + extra_cells,
            move_deep : move_deep + extent_deep + extra_cells,
        ]

    field_east = padded[:, 0]
    field_north = padded[:, 1]
    field_deep = padded[:, 2]
    flux_east = face_weight[0] * (
        region(field_deep, 0, 1, 0, 1)
        - region(field_deep, 0, 0, 0, 1)
        - (region(field_north, 0, 0, 1, 1) - region(field_north, 0, 0, 0, 1))
    )
    flux_north = face_weight[1] * (
        region(field_east, 0, 0, 1, 1)
        - region(field_east, 0, 0, 0, 1)
        - (region(field_deep, 1, 0, 0, 1) - region(field_deep, 0, 0, 0, 1))
    )
    flux_deep = face_weight[2] * (
        region(field_north, 1, 0, 0, 1)
        - region(field_north, 0, 0, 0, 1)
        - (region(field_east, 0, 1, 0, 1) - region(field_east, 0, 0, 0, 1))
    )
    out_east = (
        region(flux_north, 1, 1, 0, 0)
        - region(flux_north, 1, 1, 1, 0)
        - (region(flux_deep, 1, 0, 1, 0) - region(flux_deep, 1, 1, 1, 0))
        + masses[0] * region(field_east, 1, 1, 1, 0)
    )
    out_north = (
        region(flux_deep, 0, 1, 1, 0)
        - region(flux_deep, 1, 1, 1, 0)
        - (region(flux_east, 1, 1, 0, 0) - region(flux_east, 1, 1, 1, 0))
        + masses[1] * region(field_north, 1, 1, 1, 0)
    )
    out_deep = (
        region(flux_east, 1, 0, 1, 0)
        - region(flux_east, 1, 1, 1, 0)
        - (region(flux_north, 0, 1, 1, 0) - region(flux_north, 1, 1, 1, 0))
        + masses[2] * region(field_deep, 1, 1, 1, 0)
    )
    return jnp.stack([out_east, out_north, out_deep], axis=1)


def side_padded(plane_pad, grid_level):
    return (
        spread(grid_level[1]) * plane_pad[..., 2:, 1:-1]
        + spread(grid_level[4]) * plane_pad[..., :-2, 1:-1]
        + spread(grid_level[2]) * plane_pad[..., 1:-1, 2:]
        + spread(grid_level[5]) * plane_pad[..., 1:-1, :-2]
    )


def apply_padded(padded, grid_level):
    center = padded[:, :, 1:-1, 1:-1, 1:-1]
    along_line = (
        spread(grid_level[0]) * padded[:, :, 2:, 1:-1, 1:-1]
        + spread(grid_level[3]) * padded[:, :, :-2, 1:-1, 1:-1]
    )
    return spread(grid_level[6]) * center - (
        along_line + side_padded(padded[:, :, 1:-1], grid_level)
    )


def gradient_adjoint(padded):
    interior = padded[:, :, 1:-1, 1:-1, 1:-1]
    from_west = padded[:, 0, :-2, 1:-1, 1:-1]
    from_south = padded[:, 1, 1:-1, :-2, 1:-1]
    from_above = padded[:, 2, 1:-1, 1:-1, :-2]
    total_flow = (
        from_west - interior[:, 0] + (from_south - interior[:, 1]) + (from_above - interior[:, 2])
    )
    return total_flow[:, None]


def average_adjoint(padded):
    interior = padded[:, :, 1:-1, 1:-1, 1:-1]
    return jnp.stack(
        [
            0.5 * (interior[:, 0] + padded[:, 0, :-2, 1:-1, 1:-1]),
            0.5 * (interior[:, 1] + padded[:, 1, 1:-1, :-2, 1:-1]),
            0.5 * (interior[:, 2] + padded[:, 2, 1:-1, 1:-1, :-2]),
        ],
        axis=1,
    )


def gradient_edges(padded):
    interior = padded[:, 0, 1:-1, 1:-1, 1:-1]
    return jnp.stack(
        [
            padded[:, 0, 2:, 1:-1, 1:-1] - interior,
            padded[:, 0, 1:-1, 2:, 1:-1] - interior,
            padded[:, 0, 1:-1, 1:-1, 2:] - interior,
        ],
        axis=1,
    )


def average_edges(padded):
    return jnp.stack(
        [
            0.5 * (padded[:, 1, 1:-1, 1:-1, 1:-1] + padded[:, 1, 2:, 1:-1, 1:-1]),
            0.5 * (padded[:, 2, 1:-1, 1:-1, 1:-1] + padded[:, 2, 1:-1, 2:, 1:-1]),
            0.5 * (padded[:, 3, 1:-1, 1:-1, 1:-1] + padded[:, 3, 1:-1, 1:-1, 2:]),
        ],
        axis=1,
    )


def restrict_plane(padded):
    extent_north = padded.shape[3] - 2
    extent_deep = padded.shape[4] - 2
    halved = padded[:, :, :, 1 : extent_north + 1 : 2] + 0.5 * (
        padded[:, :, :, 0:extent_north:2] + padded[:, :, :, 2 : extent_north + 2 : 2]
    )
    return halved[..., 1 : extent_deep + 1 : 2] + 0.5 * (
        halved[..., 0:extent_deep:2] + halved[..., 2 : extent_deep + 2 : 2]
    )


def prolong_plane(padded):
    extent_north = padded.shape[3] - 2
    extent_deep = padded.shape[4] - 2
    even_rows = padded[:, :, :, 1 : extent_north + 1]
    odd_rows = 0.5 * (even_rows + padded[:, :, :, 2 : extent_north + 2])
    widened = jnp.stack([even_rows, odd_rows], axis=4)
    widened = widened.reshape(widened.shape[:3] + (2 * extent_north, extent_deep + 2))
    even_layers = widened[..., 1 : extent_deep + 1]
    odd_layers = 0.5 * (even_layers + widened[..., 2 : extent_deep + 2])
    joined = jnp.stack([even_layers, odd_layers], axis=5)
    return joined.reshape(joined.shape[:4] + (2 * extent_deep,))


def factor_lines(below_diagonal, main_diagonal, above_diagonal, entering):

    def forward(factor_before, row_items):
        below_row, main_row, above_row = row_items
        pivots = main_row - below_row * factor_before
        factor = above_row / pivots
        return (factor, (pivots, factor))

    ignored, (pivot_rows, factor_rows) = lax.scan(
        forward,
        entering,
        (
            jnp.moveaxis(below_diagonal, 1, 0),
            jnp.moveaxis(main_diagonal, 1, 0),
            jnp.moveaxis(above_diagonal, 1, 0),
        ),
    )
    return (jnp.moveaxis(pivot_rows, 0, 1), jnp.moveaxis(factor_rows, 0, 1))


def eliminate_rows(source, below_diagonal, pivots):

    def forward(earlier_row, row_items):
        below_row, pivot_row, source_row = row_items
        eliminated = (source_row - spread(below_row) * earlier_row) / spread(pivot_row)
        return (eliminated, eliminated)

    ignored, rows_out = lax.scan(
        forward,
        jnp.zeros(source[:, :, 0].shape, jnp.float32),
        (
            jnp.moveaxis(below_diagonal, 1, 0),
            jnp.moveaxis(pivots, 1, 0),
            jnp.moveaxis(source, 2, 0),
        ),
    )
    return jnp.moveaxis(rows_out, 0, 2)


def substitute_rows(eliminated, factors):

    def backward(next_value, row_items):
        factor_row, reduced_row = row_items
        solved = reduced_row - spread(factor_row) * next_value
        return (solved, solved)

    ignored, rows_out = lax.scan(
        backward,
        jnp.zeros(eliminated[:, :, 0].shape, jnp.float32),
        (jnp.moveaxis(factors, 1, 0), jnp.moveaxis(eliminated, 2, 0)),
        reverse=True,
    )
    return jnp.moveaxis(rows_out, 0, 2)


def plain_solve(right_side, below_diagonal, pivots, factors):

    def forward(earlier_row, row_items):
        below_row, pivot_row, source_row = row_items
        eliminated = (source_row - below_row * earlier_row) / pivot_row
        return (eliminated, eliminated)

    ignored, rows_out = lax.scan(
        forward,
        jnp.zeros(right_side[:, 0].shape, jnp.float32),
        (
            jnp.moveaxis(below_diagonal, 1, 0),
            jnp.moveaxis(pivots, 1, 0),
            jnp.moveaxis(right_side, 1, 0),
        ),
    )

    def backward(next_value, row_items):
        factor_row, reduced_row = row_items
        solved = reduced_row - factor_row * next_value
        return (solved, solved)

    ignored, solved_rows = lax.scan(
        backward,
        jnp.zeros(right_side[:, 0].shape, jnp.float32),
        (jnp.moveaxis(factors, 1, 0), rows_out),
        reverse=True,
    )
    return jnp.moveaxis(solved_rows, 0, 1)


def spike_level(grid_level):
    below_diagonal = -grid_level[3]
    main_diagonal = grid_level[6]
    above_diagonal = -grid_level[0]
    pivots, factors = factor_lines(
        below_diagonal,
        main_diagonal,
        above_diagonal,
        jnp.zeros(main_diagonal[:, 0].shape, jnp.float32),
    )
    inner_zero = jnp.zeros_like(main_diagonal[:, 1:])
    spike_before = plain_solve(
        jnp.concatenate([below_diagonal[:, :1], inner_zero], axis=1),
        below_diagonal,
        pivots,
        factors,
    )
    spike_after = plain_solve(
        jnp.concatenate([inner_zero, above_diagonal[:, -1:]], axis=1),
        below_diagonal,
        pivots,
        factors,
    )
    end_rows = jnp.stack(
        [spike_before[:, 0], spike_before[:, -1], spike_after[:, 0], spike_after[:, -1]], axis=1
    )
    return (
        (below_diagonal, pivots, factors, spike_before, spike_after),
        end_rows.reshape(end_rows.shape[:2] + (1, -1)),
    )


def reduce_chain(coefficients):
    before_first, before_last, after_first, after_last = (
        coefficients[:, member] for member in range(4)
    )

    def forward(beta_before, row_items):
        first_row, last_row, next_first, next_last = row_items
        denominator = 1.0 - first_row * beta_before
        scaled = next_first / denominator
        beta_after = next_last + last_row * beta_before * scaled
        return (beta_after, (denominator, scaled, beta_before, beta_after))

    ignored, outputs = lax.scan(
        forward,
        jnp.zeros(before_first[:, 0].shape, jnp.float32),
        tuple(
            (
                jnp.moveaxis(values, 1, 0)
                for values in (before_first, before_last, after_first, after_last)
            )
        ),
    )
    denominators, scaled_rows, betas_before, betas_after = (
        jnp.moveaxis(values, 0, 1) for values in outputs
    )
    return (before_first, before_last, denominators, scaled_rows, betas_before, betas_after)


def reduced_factors(fine_level, coarse_level):
    fine_data, fine_ends = spike_level(fine_level)
    coarse_data, coarse_ends = spike_level(coarse_level)
    fine_rows, coarse_rows = (
        lax.all_to_all(fine_ends, "gx", split_axis=3, concat_axis=2, tiled=True),
        lax.all_to_all(coarse_ends, "gx", split_axis=3, concat_axis=2, tiled=True),
    )
    return (fine_data + (reduce_chain(fine_rows),), coarse_data + (reduce_chain(coarse_rows),))


def reduced_solve(source, line_data):
    below_diagonal, pivots, factors, spike_before, spike_after, reduced = line_data
    local_rows = substitute_rows(eliminate_rows(source, below_diagonal, pivots), factors)
    end_values = jnp.stack([local_rows[:, :, 0], local_rows[:, :, -1]], axis=2)
    end_values = end_values.reshape(end_values.shape[:3] + (-1,))
    spread_rows = tuple((jnp.moveaxis(spread(values), 1, 0) for values in reduced))
    exchanged = lax.all_to_all(end_values, "gx", split_axis=3, concat_axis=2, tiled=True)
    paired = exchanged.reshape(
        exchanged.shape[:2] + (exchanged.shape[2] // 2, 2, exchanged.shape[3])
    )
    first_values = jnp.moveaxis(paired[:, :, :, 0], 2, 0)
    last_values = jnp.moveaxis(paired[:, :, :, 1], 2, 0)
    before_first, before_last, denominators, scaled_rows, betas_before, betas_after = spread_rows

    def forward(carried, row_items):
        first_row, last_row, couple_first, couple_last, denominator, beta_before = row_items
        leading = (first_row - couple_first * carried) / denominator
        trailing = last_row - couple_last * (carried - beta_before * leading)
        return (trailing, (leading, trailing))

    ignored, (leading_rows, trailing_rows) = lax.scan(
        forward,
        jnp.zeros(first_values[0].shape, jnp.float32),
        (first_values, last_values, before_first, before_last, denominators, betas_before),
    )

    def backward(next_first, row_items):
        leading, trailing, scaled, beta_after = row_items
        solved_first = leading - scaled * next_first
        solved_last = trailing - beta_after * next_first
        return (solved_first, (next_first, solved_last))

    ignored, (next_firsts, solved_lasts) = lax.scan(
        backward,
        jnp.zeros(first_values[0].shape, jnp.float32),
        (leading_rows, trailing_rows, scaled_rows, betas_after),
        reverse=True,
    )
    previous_lasts = jnp.concatenate([jnp.zeros_like(solved_lasts[:1]), solved_lasts[:-1]], axis=0)
    coupled = jnp.stack([previous_lasts, next_firsts], axis=1)
    coupled = jnp.moveaxis(coupled.reshape((-1,) + coupled.shape[2:]), 0, 2)
    couplings = lax.all_to_all(coupled, "gx", split_axis=2, concat_axis=3, tiled=True)
    couplings = couplings.reshape(couplings.shape[:3] + local_rows.shape[3:])
    return (
        local_rows
        - spread(spike_before) * couplings[:, :, 0:1]
        - spread(spike_after) * couplings[:, :, 1:2]
    )


def line_relax(source, line_data):
    return reduced_solve(source, line_data)


def edge_rims(values, rim_width):
    return extended(values, (("gx", 2), ("gy", 3), ("gz", 4)), rim_width)


def node_rims(values):
    return extended(values, (("gx", 2), ("gy", 3), ("gz", 4)), 1)


def coarse_plane(values):
    return node_rims(values)[:, :, 1:-1]


def cycle_body(nodal_source, fine_level, coarse_level, fine_lines, coarse_lines):
    smoothed = line_relax(nodal_source, fine_lines)
    residue = nodal_source - apply_padded(node_rims(smoothed), fine_level)
    coarse_source = restrict_plane(node_rims(residue)[:, :, 1:-1])
    correction = line_relax(coarse_source, coarse_lines)
    correction = line_relax(
        coarse_source + side_padded(coarse_plane(correction), coarse_level), coarse_lines
    )
    widened = coarse_plane(correction)
    smoothed = smoothed + prolong_plane(widened)
    return line_relax(
        nodal_source + side_padded(node_rims(smoothed)[:, :, 1:-1], fine_level), fine_lines
    )


def per_device_permutes(residual, classes, edge_mask, class_weight):
    labels = jnp.arange(class_weight.shape[0], dtype=jnp.int32).reshape(-1, 1, 1, 1)
    cell_values = jnp.sum(
        jnp.where(classes[None] == labels, class_weight.reshape(-1, 1, 1, 1), 0.0), axis=0
    )
    free_edges = (1 - edge_mask).astype(jnp.float32)
    material = jnp.concatenate([cell_values[None], free_edges], axis=0)[None]
    material_pad = edge_rims(material, 2)[0]
    masses_pad, diagonal_pad, kinds_pad = edge_coefficients(material_pad[0], material_pad[1:])
    masses = masses_pad[:, 2:-2, 2:-2, 2:-2]
    edge_diagonal = diagonal_pad[:, 2:-2, 2:-2, 2:-2]
    extent_east = residual.shape[2]
    extent_north = residual.shape[3]
    extent_deep = residual.shape[4]
    fine_level = level_from(kinds_pad, 2, 2, 2, extent_east, extent_north, extent_deep)
    coarse_level = level_from(
        coarse_weights(kinds_pad), 2, 1, 1, extent_east, extent_north // 2, extent_deep // 2
    )
    fine_lines, coarse_lines = reduced_factors(fine_level, coarse_level)
    source = residual * free_edges
    first = edge_damping * source / edge_diagonal * free_edges
    remainder = source - curl_apply(edge_rims(first, 1), masses) * free_edges
    rimmed = node_rims(remainder)
    nodal_source = jnp.concatenate([gradient_adjoint(rimmed), average_adjoint(rimmed)], axis=1)
    potential = cycle_body(nodal_source, fine_level, coarse_level, fine_lines, coarse_lines)
    rimmed = node_rims(potential)
    second = first + (gradient_edges(rimmed) + average_edges(rimmed)) * free_edges
    remainder = source - curl_apply(edge_rims(second, 1), masses) * free_edges
    return second + edge_damping * remainder / edge_diagonal * free_edges


def split_dot(left, right):
    high = left.astype(jnp.bfloat16)
    low = (left - high.astype(jnp.float32)).astype(jnp.bfloat16)
    return jnp.dot(high, right, preferred_element_type=jnp.float32) + jnp.dot(
        low, right, preferred_element_type=jnp.float32
    )


def dot_split(left, right):
    high = right.astype(jnp.bfloat16)
    low = (right - high.astype(jnp.float32)).astype(jnp.bfloat16)
    return jnp.dot(left, high, preferred_element_type=jnp.float32) + jnp.dot(
        left, low, preferred_element_type=jnp.float32
    )


UNROLL = 16


def looped(low, high, body, carry):
    return lax.fori_loop(low, high, body, carry, unroll=UNROLL if (high - low) % UNROLL == 0 else True)


def gather_kernel(
    counts, residual, classes, edge_mask, class_weight, out,
    data, mass, stiff, damp, field, nodal, sides, diagonal, inverse, east_scaled, west_scaled,
    potential, residue, coarse_weight, coarse_sides, coarse_inverse, coarse_east, coarse_west,
    coarse_source, correction, second, result, arrived,
    send_z, recv_z, send_x, recv_x, send_c, recv_c, send_out, recv_out,
):
    ngx, ngy, ngz = counts
    gx, gy, gz = (lax.axis_index(name) for name in ("gx", "gy", "gz"))
    xb, yb, zb = classes.shape
    nx, ny, nz = xb * ngx, yb * ngy, zb * ngz
    yc, zc = ny // 2, nz // 2

    barrier = pltpu.get_barrier_semaphore()
    across = {"gy": 1 - gy}
    partner = {"gz": 1 - gz}
    sides_of = ((gx > 0, gx - 1, -1), (gx < ngx - 1, gx + 1, 1))

    def signal(peer):
        pl.semaphore_signal(barrier, inc=1, device_id=peer, device_id_type=pl.DeviceIdType.MESH)

    for there, near, _ in sides_of:
        pl.when(there)(lambda near=near: signal({"gx": near}))
    signal(across)
    signal(partner)

    def block(low, size, bx, by, bz):
        return data.at[
            pl.ds(low, size),
            pl.ds(bx * xb + 1, xb),
            pl.ds(pl.multiple_of(by * yb, 8), yb),
            pl.ds(pl.multiple_of(bz * zb, 128), zb),
        ]

    own = block(0, 10, gx, gy, gz)
    labels = classes[...]
    cells = jnp.full(labels.shape, class_weight[0], jnp.float32)
    for label in range(1, class_weight.shape[0]):
        cells = jnp.where(labels == label, class_weight[label], cells)
    own[0] = cells
    own[1:4] = (1 - edge_mask[...]).astype(jnp.float32)
    own[4:7] = residual[0]
    own[7:10] = residual[1]

    pl.semaphore_wait(barrier, 2 + (gx + ngx - 1) // ngx + (2 * ngx - 2 - gx) // ngx)

    ranges = ((0, 4), (4, 6), (0, 4))
    sent = []

    def copy_of(ref, peer, send_sem, recv_sem):
        return pltpu.make_async_remote_copy(
            src_ref=ref, dst_ref=ref, send_sem=send_sem, recv_sem=recv_sem,
            device_id=peer, device_id_type=pl.DeviceIdType.MESH,
        )

    def along(kind, side, far, bx, by):
        there, near, _ = sides_of[1 - side]
        copy = copy_of(block(*ranges[kind], bx, by, gz), {"gx": near}, send_z.at[kind, side, far], recv_z.at[kind, side, far])
        return there, copy

    def slot(side, far):
        return 0 if far == 0 else 1 + side * (ngx - 1) + far - 1

    def cross(kind, side, far, bx):
        at = slot(side, far)
        return copy_of(block(*ranges[kind], bx, gy, gz), across, send_x.at[kind, at], recv_x.at[kind, at])

    def inner(kind, side, far, bx, by, row, outward):
        at = slot(side, far)
        low, size = (0, 4) if kind == 0 else (4 + 3 * ((1 - gz) if outward else gz), 3)
        return copy_of(
            block(low, size, bx, by, (gz if outward else 1 - gz)), partner, send_c.at[kind, row, at], recv_c.at[kind, row, at]
        )

    def start(copy, conditions):
        run = copy.start
        for condition in conditions:
            run = (lambda condition, run: lambda: pl.when(condition)(lambda: run() and None))(condition, run)
        run()
        sent.append((conditions, copy))

    def wait_recv(copy, condition):
        if condition is None:
            copy.wait_recv()
        else:
            pl.when(condition)(lambda: copy.wait_recv())

    def here(side, far):
        return gx >= far if side == 0 else gx + far < ngx

    def bx_of(side, far):
        return jnp.maximum(gx - far, 0) if side == 0 else jnp.minimum(gx + far, ngx - 1)

    for kind in range(2):
        for side in range(2):
            there, copy = along(kind, side, 0, gx, gy)
            start(copy, [there])
        start(cross(kind, 0, 0, gx), [])
        start(inner(kind, 0, 0, gx, gy, 0, True), [])

    zero_plane = jnp.zeros((ny, nz), jnp.float32)
    for member in range(4):
        data[member, 0] = zero_plane
        data[member, nx + 1] = zero_plane
    for member in range(3):
        field[member, 0] = zero_plane
        field[member, nx + 1] = zero_plane
    for member in range(4):
        for plane in (0, nx + 1, nx + 2):
            potential[member, plane] = zero_plane

    def z_arrival(kind, side, far, by):
        bx = bx_of(side, far)
        return copy_of(
            block(*ranges[kind], bx, by, gz), partner, send_z.at[kind, side, far - 1], recv_z.at[kind, side, far - 1]
        )

    for far in range(1, ngx):
        for kind in range(2):
            for side in range(2):
                bx = bx_of(side, far)
                seen = here(side, far)
                wait_recv(z_arrival(kind, side, far, gy), seen)
                if far < ngx - 1:
                    there, copy = along(kind, side, far, bx, gy)
                    start(copy, [seen, there])
                if kind == 1 or far > 1:
                    start(cross(kind, side, far, bx), [seen])
                start(inner(kind, side, far, bx, gy, 0, True), [seen])
            if far == 1 and kind == 0:
                copy = copy_of(block(0, 4, gx, 1 - gy, gz), across, send_x.at[0, 0], recv_x.at[0, 0])
                copy.wait_recv()
                for side in range(2):
                    there, copy = along(2, side, 0, gx, 1 - gy)
                    start(copy, [there])
                start(inner(0, 0, 0, gx, 1 - gy, 1, True), [])

    def x_arrival(kind, side, far):
        at = slot(side, far)
        return copy_of(
            block(*ranges[kind], bx_of(side, far), 1 - gy, gz), across, send_x.at[kind, at], recv_x.at[kind, at]
        )

    def take_row(kind, side, far):
        seen = here(side, far) if far else None
        if kind == 0 and far == 1:
            wait_recv(z_arrival(2, side, 1, 1 - gy), seen)
        else:
            wait_recv(x_arrival(kind, side, far), seen)
        start(inner(kind, side, far, bx_of(side, far), 1 - gy, 1, True), [seen] if far else [])

    def take_inner(kind):
        for row in range(2):
            by = gy if row == 0 else 1 - gy
            for side, far in [(0, 0)] + [(side, far) for far in range(1, ngx) for side in range(2)]:
                copy = inner(kind, side, far, bx_of(side, far), by, row, False)
                wait_recv(copy, here(side, far) if far else None)

    for side in range(2):
        take_row(0, side, 1)
    take_row(1, 0, 0)
    for side in range(2):
        take_row(1, side, 1)
    for far in range(2, ngx):
        for side in range(2):
            take_row(0, side, far)
    take_inner(0)

    mine = 4 + 3 * gz

    def edges_of(rows, layers):
        at_row = lax.broadcasted_iota(jnp.int32, (rows, layers), 0)
        at_layer = lax.broadcasted_iota(jnp.int32, (rows, layers), 1)
        masks = (at_row == 0, at_row == rows - 1, at_layer == 0, at_layer == layers - 1)

        def y_low(v):
            return jnp.where(masks[0], 0.0, pltpu.roll(v, 1, 0))

        def y_high(v):
            return jnp.where(masks[1], 0.0, pltpu.roll(v, rows - 1, 0))

        def z_low(v):
            return jnp.where(masks[2], 0.0, pltpu.roll(v, 1, 1))

        def z_high(v):
            return jnp.where(masks[3], 0.0, pltpu.roll(v, layers - 1, 1))

        return masks, y_low, y_high, z_low, z_high

    masks, y_low, y_high, z_low, z_high = edges_of(ny, nz)
    _, cy_low, cy_high, cz_low, cz_high = edges_of(yc, zc)

    def level_plane(kind, i, w1, w2, w3, carry, low_y, low_z, sides_ref, inverse_ref, east_ref, west_ref):
        west, east_before = carry
        south = low_y(w2)
        shallow = low_z(w3)
        main = (1.0 + shift_ratio) * (((((w1 + west) + w2) + south) + w3) + shallow) + shift_added
        q = 1.0 / (main - west * east_before)
        east = w1 * q
        sides_ref[kind, 0, i] = w2
        sides_ref[kind, 1, i] = south
        sides_ref[kind, 2, i] = w3
        sides_ref[kind, 3, i] = shallow
        inverse_ref[kind, i] = q
        east_ref[kind, i] = east
        west_ref[kind, i] = west * q
        return (w1, east)

    def materials(i, carry):
        c0 = data[0, i + 1]
        west = data[0, i]
        above = z_low(c0)
        south = y_low(c0)
        both = c0 + west
        averages = (
            0.25 * (((c0 + south) + above) + y_low(above)),
            0.25 * ((both + above) + z_low(west)),
            0.25 * ((both + south) + y_low(west)),
        )
        masses, strong = [], []
        for d in range(3):
            free = data[1 + d, i + 1]
            m = mass_factor[d] * averages[d] * free
            diag = stiff_weight[d] + m
            k = edge_damping * free / diag
            masses.append(m)
            strong.append(diag * free)
            mass[d, i] = m
            stiff[d, i] = strong[d]
            damp[d, i] = k
        return (
            level_plane(0, i, *masses, carry[0], y_low, z_low, sides, inverse, east_scaled, west_scaled),
            level_plane(1, i, *strong, carry[1], y_low, z_low, sides, inverse, east_scaled, west_scaled),
        )

    looped(0, nx, materials, ((zero_plane, zero_plane), (zero_plane, zero_plane)))

    for far in range(2, ngx):
        for side in range(2):
            take_row(1, side, far)

    def mat(shape, fn):
        return jnp.where(
            fn(lax.broadcasted_iota(jnp.int32, shape, 0), lax.broadcasted_iota(jnp.int32, shape, 1)), 1.0, 0.0
        )

    sum_z = mat((nz, zc), lambda r, c: r // 2 == c).astype(jnp.bfloat16)
    sum_y = mat((nx * yc, nx * ny), lambda r, c: r == c // 2).astype(jnp.bfloat16)
    rest_z = (
        mat((nz, zc), lambda r, c: r == 2 * c)
        + 0.5 * mat((nz, zc), lambda r, c: (r == 2 * c + 1) | (r == 2 * c - 1))
    ).astype(jnp.bfloat16)
    rest_y = (
        mat((nx * yc, nx * ny), lambda r, c: c == 2 * r)
        + 0.5 * mat(
            (nx * yc, nx * ny),
            lambda r, c: (c == 2 * r + 1) | ((c == 2 * r - 1) & (lax.rem(r, yc) != 0)),
        )
    ).astype(jnp.bfloat16)
    prol_z = (
        mat((zc, nz), lambda r, c: c == 2 * r)
        + 0.5 * mat((zc, nz), lambda r, c: (c == 2 * r + 1) | (c == 2 * r - 1))
    ).astype(jnp.bfloat16)
    prol_y = (
        mat((nx * ny, nx * yc), lambda r, c: r == 2 * c)
        + 0.5 * mat(
            (nx * ny, nx * yc),
            lambda r, c: (r == 2 * c + 1) | ((r == 2 * c - 1) & (lax.rem(c, yc) != 0)),
        )
    ).astype(jnp.bfloat16)

    for kind, weights in enumerate((mass, stiff)):
        for d in range(3):
            summed = dot_split(sum_y, split_dot(weights[d].reshape(nx * ny, nz), sum_z))
            factor = coarse_along if d == 0 else coarse_across
            coarse_weight[kind, d] = (factor * summed).reshape(nx, yc, zc)

    def coarse_level(i, carry):
        return tuple(
            level_plane(
                kind, i, coarse_weight[kind, 0, i], coarse_weight[kind, 1, i], coarse_weight[kind, 2, i],
                carry[kind], cy_low, cz_low, coarse_sides, coarse_inverse, coarse_east, coarse_west,
            )
            for kind in range(2)
        )

    coarse_zero = jnp.zeros((yc, zc), jnp.float32)
    looped(0, nx, coarse_level, ((coarse_zero, coarse_zero), (coarse_zero, coarse_zero)))

    take_inner(1)

    def scale(i, carry):
        for d in range(3):
            field[d, i + 1] = data[mine + d, i + 1] * damp[d, i]
        return carry

    looped(0, nx, scale, 0)

    def curl_plane(e, m, before):
        (e1, e2, e3), (next2, next3), (b2_before, b3_before) = e, m[0], before
        b1 = face_weight[0] * ((y_high(e3) - e3) - (z_high(e2) - e2))
        b2 = face_weight[1] * ((z_high(e1) - e1) - (next3 - e3))
        b3 = face_weight[2] * ((next2 - e2) - (y_high(e1) - e1))
        b1_y = jnp.where(masks[0], face_weight[0] * e3, pltpu.roll(b1, 1, 0))
        b1_z = jnp.where(masks[2], -face_weight[0] * e2, pltpu.roll(b1, 1, 1))
        b2_z = jnp.where(masks[2], face_weight[1] * e1, pltpu.roll(b2, 1, 1))
        b3_y = jnp.where(masks[0], -face_weight[2] * e1, pltpu.roll(b3, 1, 0))
        m1, m2, m3 = m[1]
        a1 = ((b2_z - b2) - (b3_y - b3)) + m1 * e1
        a2 = ((b3_before - b3) - (b1_z - b1)) + m2 * e2
        a3 = ((b1_y - b1) - (b2_before - b2)) + m3 * e3
        return (a1, a2, a3), (b2, b3)

    def faces_before(e1, e2, e3, next2, next3):
        b2 = face_weight[1] * ((z_high(e1) - e1) - (next3 - e3))
        b3 = face_weight[2] * ((next2 - e2) - (y_high(e1) - e1))
        return (b2, b3)

    def front(i, carry):
        before, rem1_before = carry
        e = tuple(field[d, i + 1] for d in range(3))
        applied, faces = curl_plane(
            e, ((field[1, i + 2], field[2, i + 2]), tuple(mass[d, i] for d in range(3))), before
        )
        r1, r2, r3 = (
            (data[mine + d, i + 1] - applied[d]) * data[1 + d, i + 1] for d in range(3)
        )
        r2_low = y_low(r2)
        r3_low = z_low(r3)
        nodal[0, i] = ((rem1_before - r1) + (r2_low - r2)) + (r3_low - r3)
        nodal[1, i] = 0.5 * (r1 + rem1_before)
        nodal[2, i] = 0.5 * (r2 + r2_low)
        nodal[3, i] = 0.5 * (r3 + r3_low)
        return (faces, r1)

    looped(
        0, nx, front,
        (faces_before(zero_plane, zero_plane, zero_plane, field[1, 1], field[2, 1]), zero_plane),
    )

    def side_sum(refs, kind, i, v, shifts):
        low_y, high_y, low_z, high_z = shifts
        return ((refs[kind, 0, i] * high_y(v) + refs[kind, 1, i] * low_y(v)) + refs[kind, 2, i] * high_z(v)) + refs[
            kind, 3, i
        ] * low_z(v)

    fine_shifts = (y_low, y_high, z_low, z_high)
    coarse_shifts = (cy_low, cy_high, cz_low, cz_high)

    def forward(i, carry):
        done = []
        for member in range(4):
            kind = min(member, 1)
            v = nodal[member, i] * inverse[kind, i] + west_scaled[kind, i] * carry[member]
            potential[member, i + 1] = v
            done.append(v)
        return tuple(done)

    def backward_residue(step, carry):
        i = nx - 1 - step
        done = []
        for member in range(4):
            kind = min(member, 1)
            v = potential[member, i + 1] + east_scaled[kind, i] * carry[member]
            potential[member, i + 1] = v
            residue[member, i] = side_sum(sides, kind, i, v, fine_shifts)
            done.append(v)
        return tuple(done)

    zeros4 = (zero_plane,) * 4
    looped(0, nx, forward, zeros4)
    looped(0, nx, backward_residue, zeros4)

    for member in range(4):
        coarse_source[member] = dot_split(
            rest_y, split_dot(residue[member].reshape(nx * ny, nz), rest_z)
        ).reshape(nx, yc, zc)

    def coarse_solve(first_time):
        def ahead(i, carry):
            done = []
            for member in range(4):
                kind = min(member, 1)
                b = coarse_source[member, i]
                if not first_time:
                    b = b + side_sum(coarse_sides, kind, i, correction[member, i], coarse_shifts)
                v = b * coarse_inverse[kind, i] + coarse_west[kind, i] * carry[member]
                correction[member, i] = v
                done.append(v)
            return tuple(done)

        def back(step, carry):
            i = nx - 1 - step
            done = []
            for member in range(4):
                v = correction[member, i] + coarse_east[min(member, 1), i] * carry[member]
                correction[member, i] = v
                done.append(v)
            return tuple(done)

        looped(0, nx, ahead, (coarse_zero,) * 4)
        looped(0, nx, back, (coarse_zero,) * 4)

    coarse_solve(True)
    for repeat in range(1):
        coarse_solve(False)

    for member in range(4):
        residue[member] = split_dot(
            dot_split(prol_y, correction[member].reshape(nx * yc, zc)), prol_z
        ).reshape(nx, ny, nz)

    def forward_again(i, carry):
        done = []
        for member in range(4):
            kind = min(member, 1)
            smoothed = potential[member, i + 1] + residue[member, i]
            b = nodal[member, i] + side_sum(sides, kind, i, smoothed, fine_shifts)
            v = b * inverse[kind, i] + west_scaled[kind, i] * carry[member]
            potential[member, i + 1] = v
            done.append(v)
        return tuple(done)

    def backward(step, carry):
        i = nx - 1 - step
        done = []
        for member in range(4):
            v = potential[member, i + 1] + east_scaled[min(member, 1), i] * carry[member]
            potential[member, i + 1] = v
            done.append(v)
        return tuple(done)

    looped(0, nx, forward_again, zeros4)
    looped(0, nx, backward, zeros4)

    base = gx * xb

    def update(step, carry):
        at = base + step
        p0, p1, p2, p3 = (potential[member, at] for member in range(4))
        second[0, step] = field[0, at] + ((potential[0, at + 1] - p0) + 0.5 * (p1 + potential[1, at + 1])) * data[1, at]
        second[1, step] = field[1, at] + ((y_high(p0) - p0) + 0.5 * (p2 + y_high(p2))) * data[2, at]
        second[2, step] = field[2, at] + ((z_high(p0) - p0) + 0.5 * (p3 + z_high(p3))) * data[3, at]
        return carry

    looped(0, xb + 2, update, 0)

    def finish(i, before):
        e = tuple(second[d, i + 1] for d in range(3))
        at = base + i
        applied, faces = curl_plane(
            e, ((second[1, i + 2], second[2, i + 2]), tuple(mass[d, at] for d in range(3))), before
        )
        for d in range(3):
            result[d, i] = e[d] + damp[d, at] * (data[mine + d, at + 1] - applied[d])
        return faces

    looped(
        0, xb, finish,
        faces_before(second[0, 0], second[1, 0], second[2, 0], second[1, 1], second[2, 1]),
    )

    def part(bz):
        return result.at[:, :, pl.ds(pl.multiple_of(gy * yb, 8), yb), pl.ds(pl.multiple_of(bz * zb, 128), zb)]

    other = 1 - gz
    swap = pltpu.make_async_remote_copy(
        src_ref=part(other), dst_ref=arrived, send_sem=send_out, recv_sem=recv_out,
        device_id={"gz": other}, device_id_type=pl.DeviceIdType.MESH,
    )
    swap.start()
    out[pl.ds(gz, 1)] = part(gz)[...][None]
    swap.wait()
    for conditions, copy in sent:
        finish_send = copy.wait_send
        for condition in conditions:
            finish_send = (lambda condition, run: lambda: pl.when(condition)(lambda: run() and None))(condition, finish_send)
        finish_send()
    out[pl.ds(other, 1)] = arrived[...][None]


def per_device(residual, classes, edge_mask, class_weight):
    counts = tuple(lax.axis_size(name) for name in ("gx", "gy", "gz"))
    ngx, ngy, ngz = counts
    xb, yb, zb = classes.shape
    nx, ny, nz = xb * ngx, yb * ngy, zb * ngz
    cells = nx * ny * nz
    aligned = yb % 8 == 0 and zb % 128 == 0 and (ny // 2) % 8 == 0 and (nz // 2) % 128 == 0
    if ngz != 2 or ngy != 2 or residual.shape[0] != 2 or not aligned or cells * 4 * 80 > 48 * 2**20:
        return per_device_permutes(residual, classes, edge_mask, class_weight)
    yc, zc = ny // 2, nz // 2

    def held(*shape):
        return pltpu.VMEM(shape, jnp.float32)

    dma = pltpu.SemaphoreType.DMA
    vmem = pl.BlockSpec(memory_space=pltpu.VMEM)
    return pl.pallas_call(
        lambda *refs: gather_kernel(counts, *refs),
        out_shape=jax.ShapeDtypeStruct(residual.shape, jnp.float32),
        in_specs=[vmem, vmem, vmem, pl.BlockSpec(memory_space=pltpu.SMEM)],
        out_specs=vmem,
        scratch_shapes=[
            held(10, nx + 2, ny, nz),
            held(3, nx, ny, nz),
            held(3, nx, ny, nz),
            held(3, nx, ny, nz),
            held(3, nx + 2, ny, nz),
            held(4, nx, ny, nz),
            held(2, 4, nx, ny, nz),
            held(1, 1, 8, 128),
            held(2, nx, ny, nz),
            held(2, nx, ny, nz),
            held(2, nx, ny, nz),
            held(4, nx + 3, ny, nz),
            held(4, nx, ny, nz),
            held(2, 3, nx, yc, zc),
            held(2, 4, nx, yc, zc),
            held(2, nx, yc, zc),
            held(2, nx, yc, zc),
            held(2, nx, yc, zc),
            held(4, nx, yc, zc),
            held(4, nx, yc, zc),
            held(3, xb + 2, ny, nz),
            held(3, xb, ny, nz),
            held(3, xb, yb, zb),
            dma((3, 2, ngx)), dma((3, 2, ngx)),
            dma((2, 2 * ngx)), dma((2, 2 * ngx)),
            dma((2, 2, 2 * ngx)), dma((2, 2, 2 * ngx)),
            dma, dma,
        ],
        compiler_params=pltpu.CompilerParams(
            collective_id=0, has_side_effects=True, vmem_limit_bytes=60 * 2**20
        ),
    )(residual, classes, edge_mask, class_weight)


def solution(mesh):
    return jax.shard_map(
        per_device,
        mesh=mesh,
        in_specs=(
            P("period", None, "gx", "gy", "gz"),
            P("gx", "gy", "gz"),
            P(None, "gx", "gy", "gz"),
            P("period"),
        ),
        out_specs=P("period", None, "gx", "gy", "gz"),
        check_vma=False,
    )
```

```python
import jax
import jax.numpy as jnp
from jax import lax
from jax.experimental import pallas as pl
from jax.experimental.pallas import tpu as pltpu
from jax.sharding import PartitionSpec as P

aspect = 2.0
face_weight = (1.0 / (aspect * aspect), 1.0, 1.0)
mass_factor = (aspect * aspect, 1.0, 1.0)
stiff_weight = (
    2.0 * (face_weight[1] + face_weight[2]),
    2.0 * (face_weight[0] + face_weight[2]),
    2.0 * (face_weight[0] + face_weight[1]),
)
edge_damping = 0.6
shift_ratio = 0.0001
shift_added = 0.05
coarse_along = 0.5625
coarse_across = 0.1875


def extended(block, sides, width):
    for axis, dim in sides:
        count = lax.axis_size(axis)
        forward = [(i, i + 1) for i in range(count - 1)]
        backward = [(target, source) for source, target in forward]
        low = lax.ppermute(
            lax.slice_in_dim(block, block.shape[dim] - width, None, axis=dim), axis, forward
        )
        high = lax.ppermute(lax.slice_in_dim(block, 0, width, axis=dim), axis, backward)
        block = jnp.concatenate([low, block, high], axis=dim)
    return block


def shifted(values, axis_index):
    axis_index = axis_index % values.ndim
    length = values.shape[axis_index]
    widths = [(0, 0)] * values.ndim
    widths[axis_index] = (1, 0)
    return lax.slice_in_dim(jnp.pad(values, widths), 0, length, axis=axis_index)


def spread(per_kind):
    scalar_kind = per_kind[0:1]
    vector_kind = per_kind[1:2]
    return jnp.concatenate([scalar_kind, vector_kind, vector_kind, vector_kind], axis=0)


def edge_coefficients(cell_values, free_edges):
    cells_west = shifted(cell_values, 0)
    cells_south = shifted(cell_values, 1)
    cells_above = shifted(cell_values, 2)
    first_edges = 0.25 * (cell_values + cells_south + cells_above + shifted(cells_above, 1))
    second_edges = 0.25 * (cell_values + cells_west + cells_above + shifted(cells_above, 0))
    third_edges = 0.25 * (cell_values + cells_west + cells_south + shifted(cells_south, 0))
    averages = jnp.stack([first_edges, second_edges, third_edges])
    factors = jnp.array(mass_factor, jnp.float32).reshape(3, 1, 1, 1)
    stiffness = jnp.array(stiff_weight, jnp.float32).reshape(3, 1, 1, 1)
    masses = factors * averages * free_edges
    edge_diagonal = stiffness + masses
    kind_weights = jnp.stack([masses, edge_diagonal * free_edges])
    return (masses, edge_diagonal, kind_weights)


def coarse_weights(kind_weights):
    grouped = kind_weights.reshape(
        kind_weights.shape[:3] + (kind_weights.shape[3] // 2, 2, kind_weights.shape[4] // 2, 2)
    )
    summed = (
        grouped[:, :, :, :, 0, :, 0]
        + grouped[:, :, :, :, 1, :, 0]
        + (grouped[:, :, :, :, 0, :, 1] + grouped[:, :, :, :, 1, :, 1])
    )
    factors = jnp.array([coarse_along, coarse_across, coarse_across], jnp.float32).reshape(
        1, 3, 1, 1, 1
    )
    return summed * factors


def level_from(
    weights_pad, start_east, start_north, start_deep, extent_east, extent_north, extent_deep
):

    def window(component, back_east, back_north, back_deep):
        low_east = start_east - back_east
        low_north = start_north - back_north
        low_deep = start_deep - back_deep
        return weights_pad[
            :,
            component,
            low_east : low_east + extent_east,
            low_north : low_north + extent_north,
            low_deep : low_deep + extent_deep,
        ]

    to_east = window(0, 0, 0, 0)
    to_north = window(1, 0, 0, 0)
    to_deep = window(2, 0, 0, 0)
    to_west = window(0, 1, 0, 0)
    to_south = window(1, 0, 1, 0)
    to_shallow = window(2, 0, 0, 1)
    weight_sum = to_east + to_west + to_north + to_south + to_deep + to_shallow
    return (
        to_east,
        to_north,
        to_deep,
        to_west,
        to_south,
        to_shallow,
        (1.0 + shift_ratio) * weight_sum + shift_added,
    )


def curl_apply(padded, masses):
    extent_east = padded.shape[2] - 2
    extent_north = padded.shape[3] - 2
    extent_deep = padded.shape[4] - 2

    def region(values, move_east, move_north, move_deep, extra_cells):
        return values[
            :,
            move_east : move_east + extent_east + extra_cells,
            move_north : move_north + extent_north + extra_cells,
            move_deep : move_deep + extent_deep + extra_cells,
        ]

    field_east = padded[:, 0]
    field_north = padded[:, 1]
    field_deep = padded[:, 2]
    flux_east = face_weight[0] * (
        region(field_deep, 0, 1, 0, 1)
        - region(field_deep, 0, 0, 0, 1)
        - (region(field_north, 0, 0, 1, 1) - region(field_north, 0, 0, 0, 1))
    )
    flux_north = face_weight[1] * (
        region(field_east, 0, 0, 1, 1)
        - region(field_east, 0, 0, 0, 1)
        - (region(field_deep, 1, 0, 0, 1) - region(field_deep, 0, 0, 0, 1))
    )
    flux_deep = face_weight[2] * (
        region(field_north, 1, 0, 0, 1)
        - region(field_north, 0, 0, 0, 1)
        - (region(field_east, 0, 1, 0, 1) - region(field_east, 0, 0, 0, 1))
    )
    out_east = (
        region(flux_north, 1, 1, 0, 0)
        - region(flux_north, 1, 1, 1, 0)
        - (region(flux_deep, 1, 0, 1, 0) - region(flux_deep, 1, 1, 1, 0))
        + masses[0] * region(field_east, 1, 1, 1, 0)
    )
    out_north = (
        region(flux_deep, 0, 1, 1, 0)
        - region(flux_deep, 1, 1, 1, 0)
        - (region(flux_east, 1, 1, 0, 0) - region(flux_east, 1, 1, 1, 0))
        + masses[1] * region(field_north, 1, 1, 1, 0)
    )
    out_deep = (
        region(flux_east, 1, 0, 1, 0)
        - region(flux_east, 1, 1, 1, 0)
        - (region(flux_north, 0, 1, 1, 0) - region(flux_north, 1, 1, 1, 0))
        + masses[2] * region(field_deep, 1, 1, 1, 0)
    )
    return jnp.stack([out_east, out_north, out_deep], axis=1)


def side_padded(plane_pad, grid_level):
    return (
        spread(grid_level[1]) * plane_pad[..., 2:, 1:-1]
        + spread(grid_level[4]) * plane_pad[..., :-2, 1:-1]
        + spread(grid_level[2]) * plane_pad[..., 1:-1, 2:]
        + spread(grid_level[5]) * plane_pad[..., 1:-1, :-2]
    )


def apply_padded(padded, grid_level):
    center = padded[:, :, 1:-1, 1:-1, 1:-1]
    along_line = (
        spread(grid_level[0]) * padded[:, :, 2:, 1:-1, 1:-1]
        + spread(grid_level[3]) * padded[:, :, :-2, 1:-1, 1:-1]
    )
    return spread(grid_level[6]) * center - (
        along_line + side_padded(padded[:, :, 1:-1], grid_level)
    )


def gradient_adjoint(padded):
    interior = padded[:, :, 1:-1, 1:-1, 1:-1]
    from_west = padded[:, 0, :-2, 1:-1, 1:-1]
    from_south = padded[:, 1, 1:-1, :-2, 1:-1]
    from_above = padded[:, 2, 1:-1, 1:-1, :-2]
    total_flow = (
        from_west - interior[:, 0] + (from_south - interior[:, 1]) + (from_above - interior[:, 2])
    )
    return total_flow[:, None]


def average_adjoint(padded):
    interior = padded[:, :, 1:-1, 1:-1, 1:-1]
    return jnp.stack(
        [
            0.5 * (interior[:, 0] + padded[:, 0, :-2, 1:-1, 1:-1]),
            0.5 * (interior[:, 1] + padded[:, 1, 1:-1, :-2, 1:-1]),
            0.5 * (interior[:, 2] + padded[:, 2, 1:-1, 1:-1, :-2]),
        ],
        axis=1,
    )


def gradient_edges(padded):
    interior = padded[:, 0, 1:-1, 1:-1, 1:-1]
    return jnp.stack(
        [
            padded[:, 0, 2:, 1:-1, 1:-1] - interior,
            padded[:, 0, 1:-1, 2:, 1:-1] - interior,
            padded[:, 0, 1:-1, 1:-1, 2:] - interior,
        ],
        axis=1,
    )


def average_edges(padded):
    return jnp.stack(
        [
            0.5 * (padded[:, 1, 1:-1, 1:-1, 1:-1] + padded[:, 1, 2:, 1:-1, 1:-1]),
            0.5 * (padded[:, 2, 1:-1, 1:-1, 1:-1] + padded[:, 2, 1:-1, 2:, 1:-1]),
            0.5 * (padded[:, 3, 1:-1, 1:-1, 1:-1] + padded[:, 3, 1:-1, 1:-1, 2:]),
        ],
        axis=1,
    )


def restrict_plane(padded):
    extent_north = padded.shape[3] - 2
    extent_deep = padded.shape[4] - 2
    halved = padded[:, :, :, 1 : extent_north + 1 : 2] + 0.5 * (
        padded[:, :, :, 0:extent_north:2] + padded[:, :, :, 2 : extent_north + 2 : 2]
    )
    return halved[..., 1 : extent_deep + 1 : 2] + 0.5 * (
        halved[..., 0:extent_deep:2] + halved[..., 2 : extent_deep + 2 : 2]
    )


def prolong_plane(padded):
    extent_north = padded.shape[3] - 2
    extent_deep = padded.shape[4] - 2
    even_rows = padded[:, :, :, 1 : extent_north + 1]
    odd_rows = 0.5 * (even_rows + padded[:, :, :, 2 : extent_north + 2])
    widened = jnp.stack([even_rows, odd_rows], axis=4)
    widened = widened.reshape(widened.shape[:3] + (2 * extent_north, extent_deep + 2))
    even_layers = widened[..., 1 : extent_deep + 1]
    odd_layers = 0.5 * (even_layers + widened[..., 2 : extent_deep + 2])
    joined = jnp.stack([even_layers, odd_layers], axis=5)
    return joined.reshape(joined.shape[:4] + (2 * extent_deep,))


def factor_lines(below_diagonal, main_diagonal, above_diagonal, entering):

    def forward(factor_before, row_items):
        below_row, main_row, above_row = row_items
        pivots = main_row - below_row * factor_before
        factor = above_row / pivots
        return (factor, (pivots, factor))

    ignored, (pivot_rows, factor_rows) = lax.scan(
        forward,
        entering,
        (
            jnp.moveaxis(below_diagonal, 1, 0),
            jnp.moveaxis(main_diagonal, 1, 0),
            jnp.moveaxis(above_diagonal, 1, 0),
        ),
    )
    return (jnp.moveaxis(pivot_rows, 0, 1), jnp.moveaxis(factor_rows, 0, 1))


def eliminate_rows(source, below_diagonal, pivots):

    def forward(earlier_row, row_items):
        below_row, pivot_row, source_row = row_items
        eliminated = (source_row - spread(below_row) * earlier_row) / spread(pivot_row)
        return (eliminated, eliminated)

    ignored, rows_out = lax.scan(
        forward,
        jnp.zeros(source[:, :, 0].shape, jnp.float32),
        (
            jnp.moveaxis(below_diagonal, 1, 0),
            jnp.moveaxis(pivots, 1, 0),
            jnp.moveaxis(source, 2, 0),
        ),
    )
    return jnp.moveaxis(rows_out, 0, 2)


def substitute_rows(eliminated, factors):

    def backward(next_value, row_items):
        factor_row, reduced_row = row_items
        solved = reduced_row - spread(factor_row) * next_value
        return (solved, solved)

    ignored, rows_out = lax.scan(
        backward,
        jnp.zeros(eliminated[:, :, 0].shape, jnp.float32),
        (jnp.moveaxis(factors, 1, 0), jnp.moveaxis(eliminated, 2, 0)),
        reverse=True,
    )
    return jnp.moveaxis(rows_out, 0, 2)


def plain_solve(right_side, below_diagonal, pivots, factors):

    def forward(earlier_row, row_items):
        below_row, pivot_row, source_row = row_items
        eliminated = (source_row - below_row * earlier_row) / pivot_row
        return (eliminated, eliminated)

    ignored, rows_out = lax.scan(
        forward,
        jnp.zeros(right_side[:, 0].shape, jnp.float32),
        (
            jnp.moveaxis(below_diagonal, 1, 0),
            jnp.moveaxis(pivots, 1, 0),
            jnp.moveaxis(right_side, 1, 0),
        ),
    )

    def backward(next_value, row_items):
        factor_row, reduced_row = row_items
        solved = reduced_row - factor_row * next_value
        return (solved, solved)

    ignored, solved_rows = lax.scan(
        backward,
        jnp.zeros(right_side[:, 0].shape, jnp.float32),
        (jnp.moveaxis(factors, 1, 0), rows_out),
        reverse=True,
    )
    return jnp.moveaxis(solved_rows, 0, 1)


def spike_level(grid_level):
    below_diagonal = -grid_level[3]
    main_diagonal = grid_level[6]
    above_diagonal = -grid_level[0]
    pivots, factors = factor_lines(
        below_diagonal,
        main_diagonal,
        above_diagonal,
        jnp.zeros(main_diagonal[:, 0].shape, jnp.float32),
    )
    inner_zero = jnp.zeros_like(main_diagonal[:, 1:])
    spike_before = plain_solve(
        jnp.concatenate([below_diagonal[:, :1], inner_zero], axis=1),
        below_diagonal,
        pivots,
        factors,
    )
    spike_after = plain_solve(
        jnp.concatenate([inner_zero, above_diagonal[:, -1:]], axis=1),
        below_diagonal,
        pivots,
        factors,
    )
    end_rows = jnp.stack(
        [spike_before[:, 0], spike_before[:, -1], spike_after[:, 0], spike_after[:, -1]], axis=1
    )
    return (
        (below_diagonal, pivots, factors, spike_before, spike_after),
        end_rows.reshape(end_rows.shape[:2] + (1, -1)),
    )


def reduce_chain(coefficients):
    before_first, before_last, after_first, after_last = (
        coefficients[:, member] for member in range(4)
    )

    def forward(beta_before, row_items):
        first_row, last_row, next_first, next_last = row_items
        denominator = 1.0 - first_row * beta_before
        scaled = next_first / denominator
        beta_after = next_last + last_row * beta_before * scaled
        return (beta_after, (denominator, scaled, beta_before, beta_after))

    ignored, outputs = lax.scan(
        forward,
        jnp.zeros(before_first[:, 0].shape, jnp.float32),
        tuple(
            (
                jnp.moveaxis(values, 1, 0)
                for values in (before_first, before_last, after_first, after_last)
            )
        ),
    )
    denominators, scaled_rows, betas_before, betas_after = (
        jnp.moveaxis(values, 0, 1) for values in outputs
    )
    return (before_first, before_last, denominators, scaled_rows, betas_before, betas_after)


def reduced_factors(fine_level, coarse_level):
    fine_data, fine_ends = spike_level(fine_level)
    coarse_data, coarse_ends = spike_level(coarse_level)
    fine_rows, coarse_rows = (
        lax.all_to_all(fine_ends, "gx", split_axis=3, concat_axis=2, tiled=True),
        lax.all_to_all(coarse_ends, "gx", split_axis=3, concat_axis=2, tiled=True),
    )
    return (fine_data + (reduce_chain(fine_rows),), coarse_data + (reduce_chain(coarse_rows),))


def reduced_solve(source, line_data):
    below_diagonal, pivots, factors, spike_before, spike_after, reduced = line_data
    local_rows = substitute_rows(eliminate_rows(source, below_diagonal, pivots), factors)
    end_values = jnp.stack([local_rows[:, :, 0], local_rows[:, :, -1]], axis=2)
    end_values = end_values.reshape(end_values.shape[:3] + (-1,))
    spread_rows = tuple((jnp.moveaxis(spread(values), 1, 0) for values in reduced))
    exchanged = lax.all_to_all(end_values, "gx", split_axis=3, concat_axis=2, tiled=True)
    paired = exchanged.reshape(
        exchanged.shape[:2] + (exchanged.shape[2] // 2, 2, exchanged.shape[3])
    )
    first_values = jnp.moveaxis(paired[:, :, :, 0], 2, 0)
    last_values = jnp.moveaxis(paired[:, :, :, 1], 2, 0)
    before_first, before_last, denominators, scaled_rows, betas_before, betas_after = spread_rows

    def forward(carried, row_items):
        first_row, last_row, couple_first, couple_last, denominator, beta_before = row_items
        leading = (first_row - couple_first * carried) / denominator
        trailing = last_row - couple_last * (carried - beta_before * leading)
        return (trailing, (leading, trailing))

    ignored, (leading_rows, trailing_rows) = lax.scan(
        forward,
        jnp.zeros(first_values[0].shape, jnp.float32),
        (first_values, last_values, before_first, before_last, denominators, betas_before),
    )

    def backward(next_first, row_items):
        leading, trailing, scaled, beta_after = row_items
        solved_first = leading - scaled * next_first
        solved_last = trailing - beta_after * next_first
        return (solved_first, (next_first, solved_last))

    ignored, (next_firsts, solved_lasts) = lax.scan(
        backward,
        jnp.zeros(first_values[0].shape, jnp.float32),
        (leading_rows, trailing_rows, scaled_rows, betas_after),
        reverse=True,
    )
    previous_lasts = jnp.concatenate([jnp.zeros_like(solved_lasts[:1]), solved_lasts[:-1]], axis=0)
    coupled = jnp.stack([previous_lasts, next_firsts], axis=1)
    coupled = jnp.moveaxis(coupled.reshape((-1,) + coupled.shape[2:]), 0, 2)
    couplings = lax.all_to_all(coupled, "gx", split_axis=2, concat_axis=3, tiled=True)
    couplings = couplings.reshape(couplings.shape[:3] + local_rows.shape[3:])
    return (
        local_rows
        - spread(spike_before) * couplings[:, :, 0:1]
        - spread(spike_after) * couplings[:, :, 1:2]
    )


def line_relax(source, line_data):
    return reduced_solve(source, line_data)


def edge_rims(values, rim_width):
    return extended(values, (("gx", 2), ("gy", 3), ("gz", 4)), rim_width)


def node_rims(values):
    return extended(values, (("gx", 2), ("gy", 3), ("gz", 4)), 1)


def coarse_plane(values):
    return node_rims(values)[:, :, 1:-1]


def cycle_body(nodal_source, fine_level, coarse_level, fine_lines, coarse_lines):
    smoothed = line_relax(nodal_source, fine_lines)
    residue = nodal_source - apply_padded(node_rims(smoothed), fine_level)
    coarse_source = restrict_plane(node_rims(residue)[:, :, 1:-1])
    correction = line_relax(coarse_source, coarse_lines)
    correction = line_relax(
        coarse_source + side_padded(coarse_plane(correction), coarse_level), coarse_lines
    )
    widened = coarse_plane(correction)
    smoothed = smoothed + prolong_plane(widened)
    return line_relax(
        nodal_source + side_padded(node_rims(smoothed)[:, :, 1:-1], fine_level), fine_lines
    )


def per_device_permutes(residual, classes, edge_mask, class_weight):
    labels = jnp.arange(class_weight.shape[0], dtype=jnp.int32).reshape(-1, 1, 1, 1)
    cell_values = jnp.sum(
        jnp.where(classes[None] == labels, class_weight.reshape(-1, 1, 1, 1), 0.0), axis=0
    )
    free_edges = (1 - edge_mask).astype(jnp.float32)
    material = jnp.concatenate([cell_values[None], free_edges], axis=0)[None]
    material_pad = edge_rims(material, 2)[0]
    masses_pad, diagonal_pad, kinds_pad = edge_coefficients(material_pad[0], material_pad[1:])
    masses = masses_pad[:, 2:-2, 2:-2, 2:-2]
    edge_diagonal = diagonal_pad[:, 2:-2, 2:-2, 2:-2]
    extent_east = residual.shape[2]
    extent_north = residual.shape[3]
    extent_deep = residual.shape[4]
    fine_level = level_from(kinds_pad, 2, 2, 2, extent_east, extent_north, extent_deep)
    coarse_level = level_from(
        coarse_weights(kinds_pad), 2, 1, 1, extent_east, extent_north // 2, extent_deep // 2
    )
    fine_lines, coarse_lines = reduced_factors(fine_level, coarse_level)
    source = residual * free_edges
    first = edge_damping * source / edge_diagonal * free_edges
    remainder = source - curl_apply(edge_rims(first, 1), masses) * free_edges
    rimmed = node_rims(remainder)
    nodal_source = jnp.concatenate([gradient_adjoint(rimmed), average_adjoint(rimmed)], axis=1)
    potential = cycle_body(nodal_source, fine_level, coarse_level, fine_lines, coarse_lines)
    rimmed = node_rims(potential)
    second = first + (gradient_edges(rimmed) + average_edges(rimmed)) * free_edges
    remainder = source - curl_apply(edge_rims(second, 1), masses) * free_edges
    return second + edge_damping * remainder / edge_diagonal * free_edges


def split_dot(left, right):
    high = left.astype(jnp.bfloat16)
    low = (left - high.astype(jnp.float32)).astype(jnp.bfloat16)
    return jnp.dot(high, right, preferred_element_type=jnp.float32) + jnp.dot(
        low, right, preferred_element_type=jnp.float32
    )


def dot_split(left, right):
    high = right.astype(jnp.bfloat16)
    low = (right - high.astype(jnp.float32)).astype(jnp.bfloat16)
    return jnp.dot(left, high, preferred_element_type=jnp.float32) + jnp.dot(
        left, low, preferred_element_type=jnp.float32
    )


UNROLL = 16


def looped(low, high, body, carry):
    return lax.fori_loop(low, high, body, carry, unroll=UNROLL if (high - low) % UNROLL == 0 else True)


def gather_kernel(
    counts, residual, classes, edge_mask, class_weight, out,
    data, mass, stiff, damp, field, nodal, sides, diagonal, inverse, east_scaled, west_scaled,
    potential, residue, coarse_weight, coarse_sides, coarse_inverse, coarse_east, coarse_west,
    coarse_source, correction, second, result, arrived,
    send_z, recv_z, send_x, recv_x, send_c, recv_c, send_out, recv_out,
):
    ngx, ngy, ngz = counts
    gx, gy, gz = (lax.axis_index(name) for name in ("gx", "gy", "gz"))
    xb, yb, zb = classes.shape
    nx, ny, nz = xb * ngx, yb * ngy, zb * ngz
    yc, zc = ny // 2, nz // 2

    barrier = pltpu.get_barrier_semaphore()
    across = {"gy": 1 - gy}
    partner = {"gz": 1 - gz}
    sides_of = ((gx > 0, gx - 1, -1), (gx < ngx - 1, gx + 1, 1))

    def signal(peer):
        pl.semaphore_signal(barrier, inc=1, device_id=peer, device_id_type=pl.DeviceIdType.MESH)

    for there, near, _ in sides_of:
        pl.when(there)(lambda near=near: signal({"gx": near}))
    signal(across)
    signal(partner)

    half = xb // 2 if xb % 2 == 0 else xb
    pieces = xb // half

    def block(low, size, bx, by, bz, piece=None):
        return data.at[
            pl.ds(low, size),
            pl.ds(bx * xb + 1, xb) if piece is None else pl.ds(bx * xb + 1 + piece * half, half),
            pl.ds(pl.multiple_of(by * yb, 8), yb),
            pl.ds(pl.multiple_of(bz * zb, 128), zb),
        ]

    own = block(0, 10, gx, gy, gz)
    labels = classes[...]
    cells = jnp.full(labels.shape, class_weight[0], jnp.float32)
    for label in range(1, class_weight.shape[0]):
        cells = jnp.where(labels == label, class_weight[label], cells)
    own[0] = cells
    own[1:4] = (1 - edge_mask[...]).astype(jnp.float32)
    own[4:7] = residual[0]
    own[7:10] = residual[1]

    pl.semaphore_wait(barrier, 2 + (gx + ngx - 1) // ngx + (2 * ngx - 2 - gx) // ngx)

    ranges = ((0, 4),) * pieces + ((4, 6),) * pieces
    sent = []

    def copy_of(ref, peer, send_sem, recv_sem):
        return pltpu.make_async_remote_copy(
            src_ref=ref, dst_ref=ref, send_sem=send_sem, recv_sem=recv_sem,
            device_id=peer, device_id_type=pl.DeviceIdType.MESH,
        )

    def along(kind, side, far, bx, by):
        there, near, _ = sides_of[1 - side]
        copy = copy_of(block(*ranges[kind], bx, by, gz, kind % pieces), {"gx": near}, send_z.at[kind, side, far], recv_z.at[kind, side, far])
        return there, copy

    def slot(side, far):
        return 0 if far == 0 else 1 + side * (ngx - 1) + far - 1

    def cross(kind, side, far, bx):
        at = slot(side, far)
        return copy_of(block(*ranges[kind], bx, gy, gz, kind % pieces), across, send_x.at[kind, at], recv_x.at[kind, at])

    def inner(kind, side, far, bx, by, row, outward):
        at = slot(side, far)
        low, size = (0, 4) if kind < pieces else (4 + 3 * ((1 - gz) if outward else gz), 3)
        return copy_of(
            block(low, size, bx, by, (gz if outward else 1 - gz), kind % pieces), partner, send_c.at[kind, row, at], recv_c.at[kind, row, at]
        )

    def start(copy, conditions):
        run = copy.start
        for condition in conditions:
            run = (lambda condition, run: lambda: pl.when(condition)(lambda: run() and None))(condition, run)
        run()
        sent.append((conditions, copy))

    def wait_recv(copy, condition):
        if condition is None:
            copy.wait_recv()
        else:
            pl.when(condition)(lambda: copy.wait_recv())

    def here(side, far):
        return gx >= far if side == 0 else gx + far < ngx

    def bx_of(side, far):
        return jnp.maximum(gx - far, 0) if side == 0 else jnp.minimum(gx + far, ngx - 1)

    for kind in range(2 * pieces):
        for side in range(2):
            there, copy = along(kind, side, 0, gx, gy)
            start(copy, [there])
        start(cross(kind, 0, 0, gx), [])
        start(inner(kind, 0, 0, gx, gy, 0, True), [])

    zero_plane = jnp.zeros((ny, nz), jnp.float32)
    for member in range(4):
        data[member, 0] = zero_plane
        data[member, nx + 1] = zero_plane
    for member in range(3):
        field[member, 0] = zero_plane
        field[member, nx + 1] = zero_plane
    for member in range(4):
        for plane in (0, nx + 1, nx + 2):
            potential[member, plane] = zero_plane

    def z_arrival(kind, side, far, by):
        bx = bx_of(side, far)
        return copy_of(
            block(*ranges[kind], bx, by, gz, kind % pieces), partner, send_z.at[kind, side, far - 1], recv_z.at[kind, side, far - 1]
        )

    def x_arrival(kind, side, far):
        at = slot(side, far)
        return copy_of(
            block(*ranges[kind], bx_of(side, far), 1 - gy, gz, kind % pieces), across, send_x.at[kind, at], recv_x.at[kind, at]
        )

    def take_row(kind, side, far):
        seen = here(side, far) if far else None
        wait_recv(x_arrival(kind, side, far), seen)
        start(inner(kind, side, far, bx_of(side, far), 1 - gy, 1, True), [seen] if far else [])

    for far in range(1, ngx):
        for kind in range(2 * pieces):
            for side in range(2):
                bx = bx_of(side, far)
                seen = here(side, far)
                wait_recv(z_arrival(kind, side, far, gy), seen)
                if far < ngx - 1:
                    there, copy = along(kind, side, far, bx, gy)
                    start(copy, [seen, there])
                if True:
                    start(cross(kind, side, far, bx), [seen])
                start(inner(kind, side, far, bx, gy, 0, True), [seen])
            if far == 1:
                take_row(kind, 0, 0)

    def take_inner(kind):
        for row in range(2):
            by = gy if row == 0 else 1 - gy
            for side, far in [(0, 0)] + [(side, far) for far in range(1, ngx) for side in range(2)]:
                copy = inner(kind, side, far, bx_of(side, far), by, row, False)
                wait_recv(copy, here(side, far) if far else None)

    for far in range(1, ngx):
        for kind in range(2 * pieces if far == 1 else pieces):
            for side in range(2):
                take_row(kind, side, far)
    for kind in range(pieces):
        take_inner(kind)

    mine = 4 + 3 * gz

    def edges_of(rows, layers):
        at_row = lax.broadcasted_iota(jnp.int32, (rows, layers), 0)
        at_layer = lax.broadcasted_iota(jnp.int32, (rows, layers), 1)
        masks = (at_row == 0, at_row == rows - 1, at_layer == 0, at_layer == layers - 1)

        def y_low(v):
            return jnp.where(masks[0], 0.0, pltpu.roll(v, 1, 0))

        def y_high(v):
            return jnp.where(masks[1], 0.0, pltpu.roll(v, rows - 1, 0))

        def z_low(v):
            return jnp.where(masks[2], 0.0, pltpu.roll(v, 1, 1))

        def z_high(v):
            return jnp.where(masks[3], 0.0, pltpu.roll(v, layers - 1, 1))

        return masks, y_low, y_high, z_low, z_high

    masks, y_low, y_high, z_low, z_high = edges_of(ny, nz)
    _, cy_low, cy_high, cz_low, cz_high = edges_of(yc, zc)

    def level_plane(kind, i, w1, w2, w3, carry, low_y, low_z, sides_ref, inverse_ref, east_ref, west_ref):
        west, east_before = carry
        south = low_y(w2)
        shallow = low_z(w3)
        main = (1.0 + shift_ratio) * (((((w1 + west) + w2) + south) + w3) + shallow) + shift_added
        q = 1.0 / (main - west * east_before)
        east = w1 * q
        sides_ref[kind, 0, i] = w2
        sides_ref[kind, 1, i] = south
        sides_ref[kind, 2, i] = w3
        sides_ref[kind, 3, i] = shallow
        inverse_ref[kind, i] = q
        east_ref[kind, i] = east
        west_ref[kind, i] = west * q
        return (w1, east)

    def materials(i, carry):
        c0 = data[0, i + 1]
        west = data[0, i]
        above = z_low(c0)
        south = y_low(c0)
        both = c0 + west
        averages = (
            0.25 * (((c0 + south) + above) + y_low(above)),
            0.25 * ((both + above) + z_low(west)),
            0.25 * ((both + south) + y_low(west)),
        )
        masses, strong = [], []
        for d in range(3):
            free = data[1 + d, i + 1]
            m = mass_factor[d] * averages[d] * free
            diag = stiff_weight[d] + m
            k = edge_damping * free / diag
            masses.append(m)
            strong.append(diag * free)
            mass[d, i] = m
            stiff[d, i] = strong[d]
            damp[d, i] = k
        return (
            level_plane(0, i, *masses, carry[0], y_low, z_low, sides, inverse, east_scaled, west_scaled),
            level_plane(1, i, *strong, carry[1], y_low, z_low, sides, inverse, east_scaled, west_scaled),
        )

    looped(0, nx, materials, ((zero_plane, zero_plane), (zero_plane, zero_plane)))

    for far in range(2, ngx):
        for kind in range(pieces, 2 * pieces):
            for side in range(2):
                take_row(kind, side, far)

    def mat(shape, fn):
        return jnp.where(
            fn(lax.broadcasted_iota(jnp.int32, shape, 0), lax.broadcasted_iota(jnp.int32, shape, 1)), 1.0, 0.0
        )

    sum_z = mat((nz, zc), lambda r, c: r // 2 == c).astype(jnp.bfloat16)
    sum_y = mat((nx * yc, nx * ny), lambda r, c: r == c // 2).astype(jnp.bfloat16)
    rest_z = (
        mat((nz, zc), lambda r, c: r == 2 * c)
        + 0.5 * mat((nz, zc), lambda r, c: (r == 2 * c + 1) | (r == 2 * c - 1))
    ).astype(jnp.bfloat16)
    rest_y = (
        mat((nx * yc, nx * ny), lambda r, c: c == 2 * r)
        + 0.5 * mat(
            (nx * yc, nx * ny),
            lambda r, c: (c == 2 * r + 1) | ((c == 2 * r - 1) & (lax.rem(r, yc) != 0)),
        )
    ).astype(jnp.bfloat16)
    prol_z = (
        mat((zc, nz), lambda r, c: c == 2 * r)
        + 0.5 * mat((zc, nz), lambda r, c: (c == 2 * r + 1) | (c == 2 * r - 1))
    ).astype(jnp.bfloat16)
    prol_y = (
        mat((nx * ny, nx * yc), lambda r, c: r == 2 * c)
        + 0.5 * mat(
            (nx * ny, nx * yc),
            lambda r, c: (r == 2 * c + 1) | ((r == 2 * c - 1) & (lax.rem(c, yc) != 0)),
        )
    ).astype(jnp.bfloat16)

    for kind, weights in enumerate((mass, stiff)):
        for d in range(3):
            summed = dot_split(sum_y, split_dot(weights[d].reshape(nx * ny, nz), sum_z))
            factor = coarse_along if d == 0 else coarse_across
            coarse_weight[kind, d] = (factor * summed).reshape(nx, yc, zc)

    def coarse_level(i, carry):
        return tuple(
            level_plane(
                kind, i, coarse_weight[kind, 0, i], coarse_weight[kind, 1, i], coarse_weight[kind, 2, i],
                carry[kind], cy_low, cz_low, coarse_sides, coarse_inverse, coarse_east, coarse_west,
            )
            for kind in range(2)
        )

    coarse_zero = jnp.zeros((yc, zc), jnp.float32)
    looped(0, nx, coarse_level, ((coarse_zero, coarse_zero), (coarse_zero, coarse_zero)))

    for kind in range(pieces, 2 * pieces):
        take_inner(kind)

    def scale(i, carry):
        for d in range(3):
            field[d, i + 1] = data[mine + d, i + 1] * damp[d, i]
        return carry

    looped(0, nx, scale, 0)

    def curl_plane(e, m, before):
        (e1, e2, e3), (next2, next3), (b2_before, b3_before) = e, m[0], before
        b1 = face_weight[0] * ((y_high(e3) - e3) - (z_high(e2) - e2))
        b2 = face_weight[1] * ((z_high(e1) - e1) - (next3 - e3))
        b3 = face_weight[2] * ((next2 - e2) - (y_high(e1) - e1))
        b1_y = jnp.where(masks[0], face_weight[0] * e3, pltpu.roll(b1, 1, 0))
        b1_z = jnp.where(masks[2], -face_weight[0] * e2, pltpu.roll(b1, 1, 1))
        b2_z = jnp.where(masks[2], face_weight[1] * e1, pltpu.roll(b2, 1, 1))
        b3_y = jnp.where(masks[0], -face_weight[2] * e1, pltpu.roll(b3, 1, 0))
        m1, m2, m3 = m[1]
        a1 = ((b2_z - b2) - (b3_y - b3)) + m1 * e1
        a2 = ((b3_before - b3) - (b1_z - b1)) + m2 * e2
        a3 = ((b1_y - b1) - (b2_before - b2)) + m3 * e3
        return (a1, a2, a3), (b2, b3)

    def faces_before(e1, e2, e3, next2, next3):
        b2 = face_weight[1] * ((z_high(e1) - e1) - (next3 - e3))
        b3 = face_weight[2] * ((next2 - e2) - (y_high(e1) - e1))
        return (b2, b3)

    def front(i, carry):
        before, rem1_before = carry
        e = tuple(field[d, i + 1] for d in range(3))
        applied, faces = curl_plane(
            e, ((field[1, i + 2], field[2, i + 2]), tuple(mass[d, i] for d in range(3))), before
        )
        r1, r2, r3 = (
            (data[mine + d, i + 1] - applied[d]) * data[1 + d, i + 1] for d in range(3)
        )
        r2_low = y_low(r2)
        r3_low = z_low(r3)
        nodal[0, i] = ((rem1_before - r1) + (r2_low - r2)) + (r3_low - r3)
        nodal[1, i] = 0.5 * (r1 + rem1_before)
        nodal[2, i] = 0.5 * (r2 + r2_low)
        nodal[3, i] = 0.5 * (r3 + r3_low)
        return (faces, r1)

    looped(
        0, nx, front,
        (faces_before(zero_plane, zero_plane, zero_plane, field[1, 1], field[2, 1]), zero_plane),
    )

    def side_sum(refs, kind, i, v, shifts):
        low_y, high_y, low_z, high_z = shifts
        return ((refs[kind, 0, i] * high_y(v) + refs[kind, 1, i] * low_y(v)) + refs[kind, 2, i] * high_z(v)) + refs[
            kind, 3, i
        ] * low_z(v)

    fine_shifts = (y_low, y_high, z_low, z_high)
    coarse_shifts = (cy_low, cy_high, cz_low, cz_high)

    def forward(i, carry):
        done = []
        for member in range(4):
            kind = min(member, 1)
            v = nodal[member, i] * inverse[kind, i] + west_scaled[kind, i] * carry[member]
            potential[member, i + 1] = v
            done.append(v)
        return tuple(done)

    def backward_residue(step, carry):
        i = nx - 1 - step
        done = []
        for member in range(4):
            kind = min(member, 1)
            v = potential[member, i + 1] + east_scaled[kind, i] * carry[member]
            potential[member, i + 1] = v
            residue[member, i] = side_sum(sides, kind, i, v, fine_shifts)
            done.append(v)
        return tuple(done)

    zeros4 = (zero_plane,) * 4
    looped(0, nx, forward, zeros4)
    looped(0, nx, backward_residue, zeros4)

    for member in range(4):
        coarse_source[member] = dot_split(
            rest_y, split_dot(residue[member].reshape(nx * ny, nz), rest_z)
        ).reshape(nx, yc, zc)

    def coarse_solve(first_time):
        def ahead(i, carry):
            done = []
            for member in range(4):
                kind = min(member, 1)
                b = coarse_source[member, i]
                if not first_time:
                    b = b + side_sum(coarse_sides, kind, i, correction[member, i], coarse_shifts)
                v = b * coarse_inverse[kind, i] + coarse_west[kind, i] * carry[member]
                correction[member, i] = v
                done.append(v)
            return tuple(done)

        def back(step, carry):
            i = nx - 1 - step
            done = []
            for member in range(4):
                v = correction[member, i] + coarse_east[min(member, 1), i] * carry[member]
                correction[member, i] = v
                done.append(v)
            return tuple(done)

        looped(0, nx, ahead, (coarse_zero,) * 4)
        looped(0, nx, back, (coarse_zero,) * 4)

    coarse_solve(True)
    for repeat in range(1):
        coarse_solve(False)

    for member in range(4):
        residue[member] = split_dot(
            dot_split(prol_y, correction[member].reshape(nx * yc, zc)), prol_z
        ).reshape(nx, ny, nz)

    def forward_again(i, carry):
        done = []
        for member in range(4):
            kind = min(member, 1)
            smoothed = potential[member, i + 1] + residue[member, i]
            b = nodal[member, i] + side_sum(sides, kind, i, smoothed, fine_shifts)
            v = b * inverse[kind, i] + west_scaled[kind, i] * carry[member]
            potential[member, i + 1] = v
            done.append(v)
        return tuple(done)

    def backward(step, carry):
        i = nx - 1 - step
        done = []
        for member in range(4):
            v = potential[member, i + 1] + east_scaled[min(member, 1), i] * carry[member]
            potential[member, i + 1] = v
            done.append(v)
        return tuple(done)

    looped(0, nx, forward_again, zeros4)
    looped(0, nx, backward, zeros4)

    base = gx * xb

    def update(step, carry):
        at = base + step
        p0, p1, p2, p3 = (potential[member, at] for member in range(4))
        second[0, step] = field[0, at] + ((potential[0, at + 1] - p0) + 0.5 * (p1 + potential[1, at + 1])) * data[1, at]
        second[1, step] = field[1, at] + ((y_high(p0) - p0) + 0.5 * (p2 + y_high(p2))) * data[2, at]
        second[2, step] = field[2, at] + ((z_high(p0) - p0) + 0.5 * (p3 + z_high(p3))) * data[3, at]
        return carry

    looped(0, xb + 2, update, 0)

    def finish(i, before):
        e = tuple(second[d, i + 1] for d in range(3))
        at = base + i
        applied, faces = curl_plane(
            e, ((second[1, i + 2], second[2, i + 2]), tuple(mass[d, at] for d in range(3))), before
        )
        for d in range(3):
            result[d, i] = e[d] + damp[d, at] * (data[mine + d, at + 1] - applied[d])
        return faces

    looped(
        0, xb, finish,
        faces_before(second[0, 0], second[1, 0], second[2, 0], second[1, 1], second[2, 1]),
    )

    def part(bz):
        return result.at[:, :, pl.ds(pl.multiple_of(gy * yb, 8), yb), pl.ds(pl.multiple_of(bz * zb, 128), zb)]

    other = 1 - gz
    swap = pltpu.make_async_remote_copy(
        src_ref=part(other), dst_ref=arrived, send_sem=send_out, recv_sem=recv_out,
        device_id={"gz": other}, device_id_type=pl.DeviceIdType.MESH,
    )
    swap.start()
    out[pl.ds(gz, 1)] = part(gz)[...][None]
    swap.wait()
    for conditions, copy in sent:
        finish_send = copy.wait_send
        for condition in conditions:
            finish_send = (lambda condition, run: lambda: pl.when(condition)(lambda: run() and None))(condition, finish_send)
        finish_send()
    out[pl.ds(other, 1)] = arrived[...][None]


def per_device(residual, classes, edge_mask, class_weight):
    counts = tuple(lax.axis_size(name) for name in ("gx", "gy", "gz"))
    ngx, ngy, ngz = counts
    xb, yb, zb = classes.shape
    nx, ny, nz = xb * ngx, yb * ngy, zb * ngz
    cells = nx * ny * nz
    aligned = yb % 8 == 0 and zb % 128 == 0 and (ny // 2) % 8 == 0 and (nz // 2) % 128 == 0
    if ngz != 2 or ngy != 2 or residual.shape[0] != 2 or not aligned or cells * 4 * 80 > 48 * 2**20:
        return per_device_permutes(residual, classes, edge_mask, class_weight)
    yc, zc = ny // 2, nz // 2

    def held(*shape):
        return pltpu.VMEM(shape, jnp.float32)

    dma = pltpu.SemaphoreType.DMA
    vmem = pl.BlockSpec(memory_space=pltpu.VMEM)
    return pl.pallas_call(
        lambda *refs: gather_kernel(counts, *refs),
        out_shape=jax.ShapeDtypeStruct(residual.shape, jnp.float32),
        in_specs=[vmem, vmem, vmem, pl.BlockSpec(memory_space=pltpu.SMEM)],
        out_specs=vmem,
        scratch_shapes=[
            held(10, nx + 2, ny, nz),
            held(3, nx, ny, nz),
            held(3, nx, ny, nz),
            held(3, nx, ny, nz),
            held(3, nx + 2, ny, nz),
            held(4, nx, ny, nz),
            held(2, 4, nx, ny, nz),
            held(1, 1, 8, 128),
            held(2, nx, ny, nz),
            held(2, nx, ny, nz),
            held(2, nx, ny, nz),
            held(4, nx + 3, ny, nz),
            held(4, nx, ny, nz),
            held(2, 3, nx, yc, zc),
            held(2, 4, nx, yc, zc),
            held(2, nx, yc, zc),
            held(2, nx, yc, zc),
            held(2, nx, yc, zc),
            held(4, nx, yc, zc),
            held(4, nx, yc, zc),
            held(3, xb + 2, ny, nz),
            held(3, xb, ny, nz),
            held(3, xb, yb, zb),
            dma((4, 2, ngx)), dma((4, 2, ngx)),
            dma((4, 2 * ngx)), dma((4, 2 * ngx)),
            dma((4, 2, 2 * ngx)), dma((4, 2, 2 * ngx)),
            dma, dma,
        ],
        compiler_params=pltpu.CompilerParams(
            collective_id=0, has_side_effects=True, vmem_limit_bytes=60 * 2**20
        ),
    )(residual, classes, edge_mask, class_weight)


def solution(mesh):
    return jax.shard_map(
        per_device,
        mesh=mesh,
        in_specs=(
            P("period", None, "gx", "gy", "gz"),
            P("gx", "gy", "gz"),
            P(None, "gx", "gy", "gz"),
            P("period"),
        ),
        out_specs=P("period", None, "gx", "gy", "gz"),
        check_vma=False,
    )
```
